256 devices in a mesh: expert: 64 (over x_lo, z, y), tensor: 4 (over x_hi, core).
Axes of the slice: x: 4 (x_hi: 2, x_lo: 2; x = x_hi * 2 + x_lo), y: 4, z: 8, core: 2. Of those that a mesh axis runs over, the one named last changes fastest.
Arguments:
- tokens: bfloat16 [8192, 2048], P('expert', 'tensor'), may hold values from -6 to 6
- grad_out: bfloat16 [8192, 2048], P('expert', 'tensor'), may hold values from -6 to 6
- route_weights: float32 [8192, 8], P('expert'), may hold values from 0.02 to 0.5
- expert_ids: int32 [8192, 8], P('expert'), may hold values from 0 to 127, all different within a row; in each aligned block of 128 rows (0 to 127, 128 to 255, ...) at most 12 rows name the same one
- gate_weight: bfloat16 [128, 2048, 768], P('expert', None, 'tensor'), may hold values from -0.125 to 0.125
- up_weight: bfloat16 [128, 2048, 768], P('expert', None, 'tensor'), may hold values from -0.125 to 0.125
- down_weight: bfloat16 [128, 768, 2048], P('expert', 'tensor'), may hold values from -0.21875 to 0.21875
- gate_adapter_first: bfloat16 [128, 2048, 64], P('expert'), may hold values from -0.125 to 0.125
- gate_adapter_second: bfloat16 [128, 64, 768], P('expert', None, 'tensor'), may hold values from -0.75 to 0.75
- up_adapter_first: bfloat16 [128, 2048, 64], P('expert'), may hold values from -0.125 to 0.125
- up_adapter_second: bfloat16 [128, 64, 768], P('expert', None, 'tensor'), may hold values from -0.75 to 0.75
- down_adapter_first: bfloat16 [128, 768, 64], P('expert', 'tensor'), may hold values from -0.21875 to 0.21875
- down_adapter_second: bfloat16 [128, 64, 2048], P('expert'), may hold values from -0.75 to 0.75
Outputs:
- grad_tokens: bfloat16 [8192, 2048], P('expert', 'tensor')
- gate_first_gradient: float32 [128, 2048, 64], P('expert', 'tensor')
- gate_second_gradient: float32 [128, 64, 768], P('expert', None, 'tensor')
- up_first_gradient: float32 [128, 2048, 64], P('expert', 'tensor')
- up_second_gradient: float32 [128, 64, 768], P('expert', None, 'tensor')
- down_first_gradient: float32 [128, 768, 64], P('expert', 'tensor')
- down_second_gradient: float32 [128, 64, 2048], P('expert', None, 'tensor')
The draws below stay inside these ranges and needn't reach their ends.
Inputs may be any that keep to these rules, and one draw needn't show every extreme that they name: `expert_ids`: each token names 8 different experts. Among the 128 rows of one device no expert is named more than 12 times, a bound that some block reaches.
All inputs are finite; a program needn't handle non-finite values.
Results may differ from the reference program's by a relative error of at most 0.012.
Values may be sent and summed in bfloat16 or wider, within the bound.
No kernel may reach another device: no remote copies, remote signals or barrier semaphores. Data moves between devices by JAX's collectives and lax.ppermute only.
A program may use at most 128 MiB of HBM per device.

```python
import math
import jax
import jax.numpy as jnp
import numpy as np
from jax import lax

D = 2048
FF = 768
TOP = 8
R = 64
TOK_DEV = 128
EXPERTS = 128
CAP = 12
TOKENS = 8192
N_EXPERT = 64
N_TENSOR = 4


def block_scale(key, extent, pieces, least, high):
    factor_of = 1.0
    for dim, blocks in pieces:
        draws = jax.random.uniform(jax.random.fold_in(jax.random.fold_in(key, 6), dim), (blocks,), jnp.float32, least / len(pieces), high / len(pieces))
        factor_of = factor_of * jnp.repeat(jnp.exp(draws), extent[dim] // blocks).reshape((-1,) + (1,) * (len(extent) - 1 - dim))
    return factor_of


def deal_out(rng, own, number, rows, number_of, top, limit, lean):
    sequence = jax.random.permutation(rng, number_of)
    crowded, common = load_shares(number_of, rows * top, limit, lean, True), load_shares(number_of, rows * top, limit, lean, False)
    places = jnp.arange(number_of)

    def named(lengths, rotation):
        used = int((lengths > 0).sum())
        fixed = max(1, used // 4)
        passed = fixed + (places - fixed + rotation * (used - fixed)) % max(1, number_of - fixed)
        return jnp.zeros((number_of,), jnp.int32).at[sequence[jnp.where(places < fixed, places, passed)]].set(jnp.asarray(lengths, jnp.int32))

    lengths = jnp.where(number % 4 == 0, named(crowded, number // 4), named(common, number - number // 4 - 1))
    mixed = jax.random.permutation(jax.random.fold_in(own, 3), number_of)
    donor, sink = mixed[0:number_of // 2 * 2:2], mixed[1:number_of // 2 * 2:2]
    slack = jnp.minimum(lengths[donor] - 1, limit - lengths[sink]) // 2
    slack = jnp.where((donor == sequence[0]) | (sink == sequence[0]) | (lengths[sink] == 0), 0, jnp.maximum(slack, 0))
    passed = jax.random.randint(jax.random.fold_in(own, 4), (number_of // 2,), 0, 1 << 20) % (slack + 1)
    lengths = lengths.at[donor].add(-passed).at[sink].add(passed)
    items = jnp.searchsorted(jnp.cumsum(lengths), jnp.arange(rows * top), side="right").astype(jnp.int32)
    table = items.reshape(top, rows).T
    table = table[jax.random.permutation(jax.random.fold_in(own, 1), rows)]
    rotation = jax.random.randint(jax.random.fold_in(own, 2), (rows, 1), 0, top)
    return jnp.take_along_axis(table, (jnp.arange(top)[None, :] + rotation) % top, axis=1)


def load_shares(number_of, total, limit, skew, full):
    portions = [(1 << 20) // math.isqrt(standing ** skew) + 1 for standing in range(1, number_of + 1)]
    largest = limit if full else min(limit, max(-(-total // number_of), total * portions[0] // sum(portions)))
    least = 1 if total - largest >= number_of - 1 else 0
    given, spare = [largest] + [least] * (number_of - 1), total - largest - least * (number_of - 1)
    while spare > 0:
        free = [i for i in range(1, number_of) if given[i] < largest] or [i for i in range(1, number_of) if given[i] < limit]
        whole, budget = sum([portions[i] for i in free]), spare
        for i in free:
            more = min(limit - given[i], max(1, budget * portions[i] // whole), spare)
            given[i] = given[i] + more
            spare = spare - more
    return np.array(given)


def bell_draw(rng, dims, deviation, reach, shards=(), kind=jnp.bfloat16):
    drawn = jax.random.normal(rng, dims, jnp.float32) * deviation
    if len(shards) > 0:
        drawn = block_scale(rng, dims, shards, -0.22, 0.18) * drawn
    return jnp.clip(drawn, min=-reach, max=reach).astype(kind)


def setup_inputs(seed: int = 0) -> dict:
    key_list = jax.random.split(jax.random.key(seed), 14)
    tokens = bell_draw(key_list[0], (TOKENS, D), 1.0, 6.0, ((0, 64), (1, 4)))
    grad_out = bell_draw(key_list[1], (TOKENS, D), 1.0, 6.0, ((0, 64), (1, 4)))
    route_weights = jnp.clip(jnp.exp(math.log(0.5) - 3.218876 * jax.random.uniform(key_list[2], (TOKENS, TOP), jnp.float32) ** block_scale(key_list[2], (TOKENS, TOP), ((0, 64),), -0.2, 0.2)), 0.02, 0.5)
    expert_ids_keys = jax.random.split(jax.random.fold_in(key_list[3], 1), TOKENS // TOK_DEV)
    expert_ids_turns = jax.random.permutation(jax.random.fold_in(key_list[3], 3), TOKENS // TOK_DEV)
    expert_ids = jax.vmap(lambda own, number: deal_out(jax.random.fold_in(key_list[3], 2), own, number, TOK_DEV, EXPERTS, TOP, CAP, 2))(expert_ids_keys, expert_ids_turns).reshape((TOKENS, TOP))
    gate_weight = bell_draw(key_list[4], (EXPERTS, D, FF), D ** -0.5, 0.125, ((0, 64), (2, 4)))
    up_weight = bell_draw(key_list[5], (EXPERTS, D, FF), D ** -0.5, 0.125, ((0, 64), (2, 4)))
    down_weight = bell_draw(key_list[6], (EXPERTS, FF, D), FF ** -0.5, 0.21875, ((0, 64), (1, 4)))
    gate_adapter_first = bell_draw(key_list[7], (EXPERTS, D, R), D ** -0.5, 0.125, ((0, 64),))
    gate_adapter_second = bell_draw(key_list[8], (EXPERTS, R, FF), R ** -0.5, 0.75, ((0, 64), (2, 4)))
    up_adapter_first = bell_draw(key_list[9], (EXPERTS, D, R), D ** -0.5, 0.125, ((0, 64),))
    up_adapter_second = bell_draw(key_list[10], (EXPERTS, R, FF), R ** -0.5, 0.75, ((0, 64), (2, 4)))
    down_adapter_first = bell_draw(key_list[11], (EXPERTS, FF, R), FF ** -0.5, 0.21875, ((0, 64), (1, 4)))
    down_adapter_second = bell_draw(key_list[12], (EXPERTS, R, D), R ** -0.5, 0.75, ((0, 64),))
    return dict(tokens=tokens, grad_out=grad_out, route_weights=route_weights, expert_ids=expert_ids, gate_weight=gate_weight, up_weight=up_weight, down_weight=down_weight, gate_adapter_first=gate_adapter_first, gate_adapter_second=gate_adapter_second, up_adapter_first=up_adapter_first, up_adapter_second=up_adapter_second, down_adapter_first=down_adapter_first, down_adapter_second=down_adapter_second)


adapter_scale = 0.5


def expert_pass(routed_input, routed_gradient, gate_weight, up_weight, down_weight, gate_adapter_first, gate_adapter_second, up_adapter_first, up_adapter_second, down_adapter_first, down_adapter_second):
    single_float = jnp.float32
    brain_float_half = jnp.bfloat16
    adapter_gate_term = jnp.dot(routed_input, gate_adapter_first, preferred_element_type=single_float).astype(brain_float_half)
    adapter_up_term = jnp.dot(routed_input, up_adapter_first, preferred_element_type=single_float).astype(brain_float_half)
    gate_activation = jnp.dot(routed_input, gate_weight, preferred_element_type=single_float) + adapter_scale * jnp.dot(adapter_gate_term, gate_adapter_second, preferred_element_type=single_float)
    up_activation = jnp.dot(routed_input, up_weight, preferred_element_type=single_float) + adapter_scale * jnp.dot(adapter_up_term, up_adapter_second, preferred_element_type=single_float)
    sigma = jax.nn.sigmoid(gate_activation)
    active = gate_activation * sigma
    hidden_activation = (active * up_activation).astype(brain_float_half)
    down_adapter_term = jnp.dot(hidden_activation, down_adapter_first, preferred_element_type=single_float).astype(brain_float_half)
    backward_adapter_term = jnp.dot(routed_gradient, down_adapter_second.T, preferred_element_type=single_float).astype(brain_float_half)
    hidden_gradient = jnp.dot(routed_gradient, down_weight.T, preferred_element_type=single_float) + adapter_scale * jnp.dot(backward_adapter_term, down_adapter_first.T, preferred_element_type=single_float)
    gate_gradient = (hidden_gradient * up_activation * sigma * (1.0 + gate_activation * (1.0 - sigma))).astype(brain_float_half)
    up_gradient = (hidden_gradient * active).astype(brain_float_half)
    gate_backward = jnp.dot(gate_gradient, gate_adapter_second.T, preferred_element_type=single_float).astype(brain_float_half)
    up_backward = jnp.dot(up_gradient, up_adapter_second.T, preferred_element_type=single_float).astype(brain_float_half)
    grads = (
        adapter_scale * jnp.dot(routed_input.T, gate_backward, preferred_element_type=single_float),
        adapter_scale * jnp.dot(adapter_gate_term.T, gate_gradient, preferred_element_type=single_float),
        adapter_scale * jnp.dot(routed_input.T, up_backward, preferred_element_type=single_float),
        adapter_scale * jnp.dot(adapter_up_term.T, up_gradient, preferred_element_type=single_float),
        adapter_scale * jnp.dot(hidden_activation.T, backward_adapter_term, preferred_element_type=single_float),
        adapter_scale * jnp.dot(down_adapter_term.T, routed_gradient, preferred_element_type=single_float),
    )
    block_width = FF // N_TENSOR
    total = jnp.zeros((routed_input.shape[0], D), single_float)
    for block in range(N_TENSOR):
        lower = block * block_width
        upper = lower + block_width
        gate_portion = jnp.dot(gate_gradient[:, lower:upper], gate_adapter_second[:, lower:upper].T, preferred_element_type=single_float).astype(brain_float_half)
        up_portion = jnp.dot(up_gradient[:, lower:upper], up_adapter_second[:, lower:upper].T, preferred_element_type=single_float).astype(brain_float_half)
        merged_result = jnp.dot(gate_gradient[:, lower:upper], gate_weight[:, lower:upper].T, preferred_element_type=single_float)
        merged_result = merged_result + jnp.dot(up_gradient[:, lower:upper], up_weight[:, lower:upper].T, preferred_element_type=single_float)
        merged_result = merged_result + adapter_scale * (jnp.dot(gate_portion, gate_adapter_first.T, preferred_element_type=single_float) + jnp.dot(up_portion, up_adapter_first.T, preferred_element_type=single_float))
        total = total + merged_result.astype(brain_float_half).astype(single_float)
    return grads, total


def reference(tokens, grad_out, route_weights, expert_ids, gate_weight, up_weight, down_weight, gate_adapter_first, gate_adapter_second, up_adapter_first, up_adapter_second, down_adapter_first, down_adapter_second):
    single_float = jnp.float32
    brain_float_half = jnp.bfloat16
    blocks = expert_ids.reshape(N_EXPERT, TOK_DEV, TOP)
    numbers = jnp.arange(EXPERTS, dtype=jnp.int32)
    picked = jnp.any(blocks[:, :, :, None] == numbers[None, None, None, :], axis=2).astype(jnp.int32)
    before = jnp.cumsum(picked, axis=1) - picked
    slot_index = jnp.take_along_axis(before, blocks, axis=2).astype(jnp.int32)
    source = jnp.broadcast_to(jnp.arange(N_EXPERT, dtype=jnp.int32)[:, None, None], blocks.shape)
    assigned = jnp.arange(TOKENS * TOP, dtype=jnp.int32).reshape(blocks.shape)
    sentinel = TOKENS * TOP
    table = jnp.full((N_EXPERT, EXPERTS, CAP), sentinel, jnp.int32).at[source, blocks, slot_index].set(assigned)
    per_expert = jnp.transpose(table, (1, 0, 2)).reshape(EXPERTS, N_EXPERT * CAP)
    flat_weights = route_weights.reshape(-1)

    def step(accum, items):
        index, wg, wu, wd, ag, bg, au, bu, ad, bd = items
        live = index < sentinel
        safe = jnp.minimum(index, sentinel - 1)
        token_row = (safe // TOP).astype(jnp.int32)
        routed_input = jnp.where(live[:, None], tokens[token_row].astype(single_float), 0.0).astype(brain_float_half)
        factor = jnp.where(live, flat_weights[safe], 0.0)
        routed_gradient = (factor[:, None] * grad_out[token_row].astype(single_float)).astype(brain_float_half)
        grads, total = expert_pass(routed_input, routed_gradient, wg, wu, wd, ag, bg, au, bu, ad, bd)
        accum = accum.at[token_row].add(jnp.where(live[:, None], total, 0.0))
        return accum, grads

    accum, grads = lax.scan(step, jnp.zeros((TOKENS, D), single_float), (per_expert, gate_weight, up_weight, down_weight, gate_adapter_first, gate_adapter_second, up_adapter_first, up_adapter_second, down_adapter_first, down_adapter_second))
    return (accum.astype(brain_float_half), grads[0], grads[1], grads[2], grads[3], grads[4], grads[5])
```

```python
import jax
import jax.numpy as jnp
from jax import lax
from jax.sharding import PartitionSpec as P


bf16 = jnp.bfloat16
f32 = jnp.float32
SCALE = 0.5
NZ, NY, CAP = 8, 4, 12
AXES = ("expert", "tensor")


def pairs(fn):
    out = []
    for xl in range(2):
        for z in range(NZ):
            for y in range(NY):
                for xh in range(2):
                    for c in range(2):
                        a, b, d, e, f = fn(xl, z, y, xh, c)
                        src = ((xl * NZ + z) * NY + y) * 4 + xh * 2 + c
                        dst = ((a * NZ + b) * NY + d) * 4 + e * 2 + f
                        out.append((src, dst))
    return out


def inverse(perm):
    return [(d, s) for s, d in perm]


Z_BY = [pairs(lambda xl, z, y, xh, c, s=s: (xl, (z + s) % NZ, y, xh, c)) for s in range(NZ)]
Y_BY = [pairs(lambda xl, z, y, xh, c, s=s: (xl, z, (y + s) % NY, xh, c)) for s in range(NY)]
X_BY = [
    pairs(lambda xl, z, y, xh, c, i=i, j=j: (c ^ j, z, y, xh ^ i, xl))
    for i in range(2)
    for j in range(2)
]
X_HALF = pairs(lambda xl, z, y, xh, c: (xl, z, y, 1 - xh, c))
CORE = pairs(lambda xl, z, y, xh, c: (xl, z, y, xh, 1 - c))


def move(x, perm):
    return lax.ppermute(x, AXES, perm)


def dot(a, b, ca, cb):
    return lax.dot_general(a, b, (((ca,), (cb,)), ((), ())), preferred_element_type=f32)


def pick(array, index):
    return lax.dynamic_index_in_dim(array, index, 0, keepdims=False)


def natural(parts, xh, xl):
    out = []
    for a in range(2):
        for b in range(2):
            low = jnp.where(xl == 1, parts[2 * a + (1 - b)], parts[2 * a + b])
            high = jnp.where(xl == 1, parts[2 * (1 - a) + (1 - b)], parts[2 * (1 - a) + b])
            out.append(jnp.where(xh == 1, high, low))
    return out


def local(
    tokens,
    grad_out,
    route_weights,
    expert_ids,
    gate_weight,
    up_weight,
    down_weight,
    gate_adapter_first,
    gate_adapter_second,
    up_adapter_first,
    up_adapter_second,
    down_adapter_first,
    down_adapter_second,
):
    e_index = lax.axis_index("expert")
    t_index = lax.axis_index("tensor")
    xl = e_index // (NZ * NY)
    z = (e_index // NY) % NZ
    y = e_index % NY
    xh = t_index // 2
    c = t_index % 2
    rows, width = tokens.shape

    gate_t = jnp.swapaxes(gate_weight, 1, 2)
    up_t = jnp.swapaxes(up_weight, 1, 2)
    first_t = jnp.swapaxes(down_adapter_first, 1, 2)
    big = [pick(w, 1 - xh) for w in (gate_t, up_t, down_weight)]
    small = jnp.concatenate(
        [pick(w, 1 - xh) for w in (gate_adapter_second, up_adapter_second, first_t)], axis=0
    )
    big_own = [pick(w, xh) for w in (gate_t, up_t, down_weight)]
    small_own = jnp.concatenate(
        [pick(w, xh) for w in (gate_adapter_second, up_adapter_second, first_t)], axis=0
    )
    big_x = [move(w, X_HALF) for w in big]
    small_x = move(small, X_HALF)
    big_c = [move(w, CORE) for w in big_own]
    small_c = move(small_own, CORE)
    big_xc = [move(w, CORE) for w in big_x]
    small_xc = move(small_x, CORE)
    gate_w, up_w, down_w = (
        jnp.concatenate(four, axis=0) for four in zip(big_own, big_x, big_c, big_xc)
    )
    seconds = jnp.concatenate((small_own, small_x, small_c, small_xc), axis=1)
    gate_second, up_second, down_first = seconds[:64], seconds[64:128], seconds[128:]
    gate_first = pick(jnp.swapaxes(gate_adapter_first, 1, 2), xh)
    up_first = pick(jnp.swapaxes(up_adapter_first, 1, 2), xh)
    down_second = pick(down_adapter_second, xh)

    ids_t = expert_ids.T.astype(bf16)
    w_t = route_weights.T
    w_hi = lax.reduce_precision(w_t, 8, 7)
    w_rest = w_t - w_hi
    w_mid = lax.reduce_precision(w_rest, 8, 7)
    w_low = w_rest - w_mid
    meta = jnp.concatenate(
        (ids_t, w_hi.astype(bf16), w_mid.astype(bf16), w_low.astype(bf16)), axis=1
    )
    packed = jnp.concatenate((tokens, meta), axis=0)
    all_packed = [packed] + [move(packed, Z_BY[s]) for s in range(1, NZ)]
    all_grad = [grad_out] + [move(grad_out, Z_BY[s]) for s in range(1, NZ)]
    metas = [p[rows:].astype(f32) for p in all_packed]
    ids = jnp.concatenate([m[:, :rows] for m in metas], axis=1)
    weight = jnp.concatenate(
        [
            m[:, rows : 2 * rows] + m[:, 2 * rows : 3 * rows] + m[:, 3 * rows :]
            for m in metas
        ],
        axis=1,
    )

    q = lax.broadcasted_iota(jnp.int32, (16, 1), 0)
    q_y = (y + q // 4) % NY
    q_xh = xh ^ ((q // 2) % 2)
    q_xl = c ^ (q % 2)
    number = (2 * ((q_xl * NZ + z) * NY + q_y) + q_xh).astype(f32)
    match = ids[:, None, :] == number[None, :, :]
    picked = jnp.any(match, axis=0)
    slot_weight = jnp.sum(jnp.where(match, weight[:, None, :], 0.0), axis=0)
    earlier = (
        lax.broadcasted_iota(jnp.int32, (rows, rows), 0)
        < lax.broadcasted_iota(jnp.int32, (rows, rows), 1)
    ).astype(bf16)
    before = dot(picked.astype(bf16).reshape(16 * NZ, rows), earlier, 1, 0).reshape(16, NZ * rows)
    block = (lax.broadcasted_iota(jnp.int32, (1, NZ * rows), 1) // rows).astype(f32)
    target = jnp.where(picked, before + CAP * block, -1.0)
    group = NZ * CAP
    place = lax.broadcasted_iota(jnp.int32, (1, group, 1), 1).astype(f32)
    hit = target[:, None, :] == place
    select = hit.astype(bf16).reshape(16 * group, NZ * rows)
    row_weight = jnp.sum(jnp.where(hit, slot_weight[:, None, :], 0.0), axis=2).reshape(-1, 1)

    chunk = 4 * group

    def to_expert(routed):
        got = [routed[:chunk]] + [
            move(routed[s * chunk : (s + 1) * chunk], Y_BY[s]) for s in range(1, NY)
        ]
        return [
            move(
                jnp.concatenate([g[k * group : (k + 1) * group] for g in got], axis=0), X_BY[k]
            )
            for k in range(4)
        ]

    every_token = jnp.concatenate([p[:rows] for p in all_packed], axis=0)
    routed_in = dot(select, every_token, 1, 0).astype(bf16)
    in_parts = to_expert(routed_in)
    every_grad = jnp.concatenate(all_grad, axis=0)
    routed_grad = (dot(select, every_grad, 1, 0) * row_weight).astype(bf16)
    grad_parts = to_expert(routed_grad)

    routed = jnp.concatenate(natural(in_parts, xh, xl), axis=1)
    cotangent = jnp.concatenate(natural(grad_parts, xh, xl), axis=1)
    lora_gate = dot(routed, gate_first, 1, 1).astype(bf16)
    lora_up = dot(routed, up_first, 1, 1).astype(bf16)
    gate = dot(routed, gate_w, 1, 1) + SCALE * dot(lora_gate, gate_second, 1, 0)
    up = dot(routed, up_w, 1, 1) + SCALE * dot(lora_up, up_second, 1, 0)
    sigma = jax.nn.sigmoid(gate)
    active = gate * sigma
    hidden = (active * up).astype(bf16)
    down_lora = dot(hidden, down_first, 1, 1).astype(bf16)
    back_lora = dot(cotangent, down_second, 1, 1).astype(bf16)
    grad_hidden = dot(cotangent, down_w, 1, 1) + SCALE * dot(back_lora, down_first, 1, 0)
    grad_gate = (grad_hidden * up * sigma * (1.0 + gate * (1.0 - sigma))).astype(bf16)
    grad_up = (grad_hidden * active).astype(bf16)
    gate_back = dot(grad_gate, gate_second, 1, 1).astype(bf16)
    up_back = dot(grad_up, up_second, 1, 1).astype(bf16)
    input_grad = dot(grad_gate, gate_w, 1, 0) + dot(grad_up, up_w, 1, 0)
    input_grad = input_grad + SCALE * (
        dot(gate_back, gate_first, 1, 0) + dot(up_back, up_first, 1, 0)
    )
    input_grad = input_grad.astype(bf16)

    by_feature = SCALE * jnp.concatenate(
        (dot(gate_back, routed, 0, 0), dot(up_back, routed, 0, 0), dot(down_lora, cotangent, 0, 0)),
        axis=0,
    )
    by_hidden = SCALE * jnp.concatenate(
        (dot(lora_gate, grad_gate, 0, 0), dot(lora_up, grad_up, 0, 0), dot(back_lora, hidden, 0, 0)),
        axis=0,
    )

    def feature(xh_of, c_of):
        return lax.dynamic_slice_in_dim(by_feature, (2 * xh_of + c_of) * width, width, 1)

    units = gate_weight.shape[2]
    mine = jnp.concatenate(
        (feature(xh, c), feature(1 - xh, c), by_hidden[:, : 2 * units]), axis=1
    )
    other = jnp.concatenate(
        (feature(xh, 1 - c), feature(1 - xh, 1 - c), by_hidden[:, 2 * units :]), axis=1
    )
    total = mine + move(other, CORE)
    keep = jnp.concatenate(
        (total[:, :width], total[:, 2 * width : 2 * width + units]), axis=1
    )
    give = jnp.concatenate((total[:, width : 2 * width], total[:, 2 * width + units :]), axis=1)
    came = move(give, X_HALF)
    first = jnp.where(xh == 0, keep, came)
    second = jnp.where(xh == 0, came, keep)
    both = jnp.stack((first, second), axis=0)
    f_part, h_part = both[:, :, :width], both[:, :, width:]

    home = [
        move(
            lax.dynamic_slice_in_dim(
                input_grad, (2 * (xh ^ (k // 2)) + (xl ^ (k % 2))) * width, width, 1
            ),
            inverse(X_BY[k]),
        )
        for k in range(4)
    ]
    came_y = []
    for s in range(NY):
        piece = jnp.concatenate([h[s * group : (s + 1) * group] for h in home], axis=0)
        came_y.append(piece if s == 0 else move(piece, inverse(Y_BY[s])))
    slots = jnp.concatenate(came_y, axis=0)
    combined = dot(select, slots, 0, 0)
    result = combined[:rows]
    for s in range(1, NZ):
        result = result + move(
            combined[s * rows : (s + 1) * rows].astype(bf16), inverse(Z_BY[s])
        ).astype(f32)
    return (
        result.astype(bf16),
        jnp.swapaxes(f_part[:, :64], 1, 2),
        h_part[:, :64],
        jnp.swapaxes(f_part[:, 64:128], 1, 2),
        h_part[:, 64:128],
        jnp.swapaxes(h_part[:, 128:], 1, 2),
        f_part[:, 128:],
    )


def solution(mesh):
    return jax.shard_map(
        local,
        mesh=mesh,
        in_specs=(
            P("expert", "tensor"),
            P("expert", "tensor"),
            P("expert", None),
            P("expert", None),
            P("expert", None, "tensor"),
            P("expert", None, "tensor"),
            P("expert", "tensor", None),
            P("expert", None, None),
            P("expert", None, "tensor"),
            P("expert", None, None),
            P("expert", None, "tensor"),
            P("expert", "tensor", None),
            P("expert", None, None),
        ),
        out_specs=(
            P("expert", "tensor"),
            P("expert", "tensor", None),
            P("expert", None, "tensor"),
            P("expert", "tensor", None),
            P("expert", None, "tensor"),
            P("expert", "tensor", None),
            P("expert", None, "tensor"),
        ),
        check_vma=False,
    )
```

```python
import jax
import jax.numpy as jnp
from jax import lax
from jax.experimental import pallas as pl
from jax.experimental.pallas import tpu as pltpu
from jax.sharding import PartitionSpec as P


bf16 = jnp.bfloat16
f32 = jnp.float32
SCALE = 0.5
NZ, NY, CAP, TOP = 8, 4, 12, 8
AXES = ("expert", "tensor")
HALF = CAP * NZ // 2


def pairs(fn):
    out = []
    for xl in range(2):
        for z in range(NZ):
            for y in range(NY):
                for xh in range(2):
                    for c in range(2):
                        a, b, d, e, f = fn(xl, z, y, xh, c)
                        src = ((xl * NZ + z) * NY + y) * 4 + xh * 2 + c
                        dst = ((a * NZ + b) * NY + d) * 4 + e * 2 + f
                        out.append((src, dst))
    return out


def inverse(perm):
    return [(d, s) for s, d in perm]


Z_BY = [pairs(lambda xl, z, y, xh, c, s=s: (xl, (z + s) % NZ, y, xh, c)) for s in range(NZ)]
Y_BY = [pairs(lambda xl, z, y, xh, c, s=s: (xl, z, (y + s) % NY, xh, c)) for s in range(NY)]
X_BY = [
    pairs(lambda xl, z, y, xh, c, i=i, j=j: (xl ^ j, z, y, xh ^ i, c))
    for i in range(2)
    for j in range(2)
]
X_HALF = pairs(lambda xl, z, y, xh, c: (xl, z, y, 1 - xh, c))
CORE = pairs(lambda xl, z, y, xh, c: (xl, z, y, xh, 1 - c))


def move(x, perm):
    return lax.ppermute(x, AXES, perm)


def dot(a, b, ca, cb):
    return lax.dot_general(a, b, (((ca,), (cb,)), ((), ())), preferred_element_type=f32)


def pick(array, index):
    return lax.dynamic_index_in_dim(array, index, 0, keepdims=False)


VMEM = pl.BlockSpec(memory_space=pltpu.VMEM)


def select_kernel(scalars, *refs):
    packed, (*outs, target_ref, slot_weight_ref) = refs[:NZ], refs[NZ:]
    select_refs, weight_refs, out_refs = outs[:2], outs[2:4], outs[4:]
    rows = packed[0].shape[0] - TOP
    q = lax.broadcasted_iota(jnp.int32, (16, rows), 0)
    q_y = jnp.bitwise_and(scalars[6] + jnp.right_shift(q, 2), NY - 1)
    q_xh = jnp.bitwise_xor(scalars[0], jnp.bitwise_and(jnp.right_shift(q, 1), 1))
    q_xl = jnp.bitwise_xor(scalars[8], jnp.bitwise_and(q, 1))
    number = (2 * ((q_xl * NZ + scalars[7]) * NY + q_y) + q_xh).astype(f32)
    earlier = (
        lax.broadcasted_iota(jnp.int32, (rows, rows), 0)
        < lax.broadcasted_iota(jnp.int32, (rows, rows), 1)
    ).astype(f32).astype(bf16)
    for b in range(NZ):
        meta = packed[b][rows:, :].astype(f32)
        ids = meta[:, :rows]
        weight = meta[:, rows : 2 * rows] + meta[:, 2 * rows : 3 * rows] + meta[:, 3 * rows :]
        picked = jnp.zeros(number.shape, f32)
        slot_weight = jnp.zeros(number.shape, f32)
        for k in range(TOP):
            match = ids[k : k + 1, :] == number
            picked = jnp.where(match, 1.0, picked)
            slot_weight = jnp.where(match, weight[k : k + 1, :], slot_weight)
        before = dot(picked.astype(bf16), earlier, 1, 0)
        target = jnp.where(picked > 0.0, before + float(CAP * (b % 4)), -1.0)
        for q in range(16):
            target_ref[q, :, b * rows : (b + 1) * rows] = target[q : q + 1, :]
            slot_weight_ref[q, :, b * rows : (b + 1) * rows] = slot_weight[q : q + 1, :]
    place = lax.broadcasted_iota(jnp.int32, (HALF, rows), 0).astype(f32)

    def expert(q, _):
        start = pl.multiple_of(q * HALF, HALF)
        for h in range(2):
            total = jnp.zeros((HALF, rows), f32)
            for b in range(4):
                lanes = slice((4 * h + b) * rows, (4 * h + b + 1) * rows)
                hit = target_ref[q, :, lanes] == place
                select_refs[h][pl.ds(start, HALF), b * rows : (b + 1) * rows] = jnp.where(
                    hit, 1.0, 0.0
                ).astype(bf16)
                total = total + jnp.where(hit, slot_weight_ref[q, :, lanes], 0.0)
            weight_refs[h][pl.ds(start, HALF), :] = jnp.broadcast_to(
                jnp.sum(total, axis=1, keepdims=True), (HALF, rows)
            )
        return 0

    lax.fori_loop(0, 16, expert, 0)
    for h in range(2):
        every = jnp.concatenate([p[:rows, :] for p in packed[4 * h : 4 * h + 4]], axis=0)
        for s in range(NY):
            part = dot(select_refs[h][s * 4 * HALF : (s + 1) * 4 * HALF, :], every, 1, 0)
            out_refs[s][h * 4 * HALF : (h + 1) * 4 * HALF, :] = part.astype(bf16)


def select_in(scalars, packed, rows, width):
    slots = 16 * HALF
    shapes = [((slots, 4 * rows), bf16)] * 2 + [((slots, rows), f32)] * 2
    shapes += [((8 * HALF, width), bf16)] * NY
    return pl.pallas_call(
        select_kernel,
        in_specs=[SCALARS] + [VMEM] * NZ,
        out_specs=[VMEM] * len(shapes),
        out_shape=[jax.ShapeDtypeStruct(shape, dtype) for shape, dtype in shapes],
        scratch_shapes=[pltpu.VMEM((16, 1, NZ * rows), f32), pltpu.VMEM((16, 1, NZ * rows), f32)],
        name="select_in",
    )(scalars, *packed)


def select_grad_kernel(*refs):
    select_refs, weight_refs, grads, out_refs = refs[:2], refs[2:4], refs[4 : 4 + NZ], refs[4 + NZ :]
    for h in range(2):
        every = jnp.concatenate([g[...] for g in grads[4 * h : 4 * h + 4]], axis=0)
        for s in range(NY):
            part = slice(s * 4 * HALF, (s + 1) * 4 * HALF)
            product = dot(select_refs[h][part, :], every, 1, 0) * weight_refs[h][part, :1]
            out_refs[s][h * 4 * HALF : (h + 1) * 4 * HALF, :] = product.astype(bf16)


def select_grad(selects, weights, grads, width):
    return pl.pallas_call(
        select_grad_kernel,
        in_specs=[VMEM] * (4 + NZ),
        out_specs=[VMEM] * NY,
        out_shape=[jax.ShapeDtypeStruct((8 * HALF, width), bf16) for _ in range(NY)],
        name="select_grad",
    )(*selects, *weights, *grads)


def combine_kernel(*refs):
    select_refs, pieces, (down_ref, up_ref, far_ref, near_ref) = refs[:2], refs[2:6], refs[6:]
    half = near_ref.shape[0] // 3
    for h in (1, 0):
        values = jnp.concatenate(
            [p[h * 4 * HALF : (h + 1) * 4 * HALF, :] for p in pieces], axis=0
        )
        total = dot(select_refs[h][...], values, 0, 0)
        if h == 1:
            down_ref[...] = total[: 2 * half, :].astype(bf16)
            up_ref[...] = total[2 * half :, :].astype(bf16)
        else:
            near_ref[...] = total[: 3 * half, :]
            far_ref[...] = total[3 * half :, :].astype(bf16)


def combine(selects, pieces, rows, width):
    shapes = [((2 * rows, width), bf16)] * 2 + [((rows, width), bf16), ((3 * rows, width), f32)]
    return pl.pallas_call(
        combine_kernel,
        in_specs=[VMEM] * 6,
        out_specs=[VMEM] * 4,
        out_shape=[jax.ShapeDtypeStruct(shape, dtype) for shape, dtype in shapes],
        name="combine",
    )(*selects, *pieces)


SCALARS = pl.BlockSpec(memory_space=pltpu.SMEM)


def to_chips_kernel(*refs):
    for s in range(NY):
        for h in range(2):
            for k in range(4):
                refs[4 + k][(2 * s + h) * HALF : (2 * s + h + 1) * HALF, :] = refs[s][
                    (4 * h + k) * HALF : (4 * h + k + 1) * HALF, :
                ]


def from_chips_kernel(*refs):
    for s in range(NY):
        for h in range(2):
            for k in range(4):
                refs[4 + s][(4 * h + k) * HALF : (4 * h + k + 1) * HALF, :] = refs[k][
                    (2 * s + h) * HALF : (2 * s + h + 1) * HALF, :
                ]


def regroup(kernel, pieces):
    return pl.pallas_call(
        kernel,
        in_specs=[VMEM] * 4,
        out_specs=[VMEM] * 4,
        out_shape=[jax.ShapeDtypeStruct(p.shape, p.dtype) for p in pieces],
    )(*pieces)


def split_kernel(scalars, *refs):
    sent, (cross_ref, kept_0, kept_1) = refs[:4], refs[4:]
    n = kept_0.shape[0]
    for swapped in range(2):

        @pl.when(scalars[5] == swapped)
        def _(swapped=swapped):
            for i, kept in enumerate((kept_0, kept_1)):
                kept[...] = sent[2 * i + swapped][...]
                cross_ref[i * n : (i + 1) * n, :] = sent[2 * i + 1 - swapped][...]


def split(scalars, sent):
    n, width = sent[0].shape
    shapes = [(2 * n, width), (n, width), (n, width)]
    return pl.pallas_call(
        split_kernel,
        in_specs=[SCALARS] + [VMEM] * 4,
        out_specs=[VMEM] * 3,
        out_shape=[jax.ShapeDtypeStruct(shape, bf16) for shape in shapes],
        name="split_cores",
    )(scalars, *sent)


def join_kernel(scalars, own_ref, crossed_ref, *home):
    for swapped in range(2):

        @pl.when(scalars[5] == swapped)
        def _(swapped=swapped):
            for i in range(2):
                home[2 * i + swapped][...] = own_ref[i]
                home[2 * i + 1 - swapped][...] = crossed_ref[i]


def join(scalars, own, crossed):
    return pl.pallas_call(
        join_kernel,
        in_specs=[SCALARS, VMEM, VMEM],
        out_specs=[VMEM] * 4,
        out_shape=[jax.ShapeDtypeStruct(own.shape[1:], bf16)] * 4,
        name="join_cores",
    )(scalars, own, crossed)


def whole(shape):
    return pl.BlockSpec(shape, lambda g, s: (0,) * len(shape))


def stack(refs):
    return jnp.concatenate([r[0] if len(r.shape) == 3 else r[...] for r in refs], axis=0)


def forward_kernel(scalars, *refs):
    parts, (gates, ups, firsts), seconds = refs[:4], (refs[4:8], refs[8:12], refs[12:14]), refs[14]
    gate_ref, up_ref, hidden_ref, lora_gate_ref, lora_up_ref, down_lora_ref, acc = refs[15:]
    step = pl.program_id(0)
    rank = seconds.shape[0] // 3
    units = seconds.shape[1]
    weights = stack((*gates, *ups, *firsts))
    for k in range(4):

        @pl.when(step == k)
        def _(k=k):
            product = dot(parts[k][...], weights, 1, 1)
            acc[...] = product if k == 0 else acc[...] + product

    @pl.when(step == 3)
    def _():
        lora_gate = acc[:, 2 * units : 2 * units + rank].astype(bf16)
        lora_up = acc[:, 2 * units + rank :].astype(bf16)
        gate = acc[:, :units] + SCALE * dot(lora_gate, seconds[:rank, :], 1, 0)
        up = acc[:, units : 2 * units] + SCALE * dot(lora_up, seconds[rank : 2 * rank, :], 1, 0)
        hidden = (gate * jax.nn.sigmoid(gate) * up).astype(bf16)
        gate_ref[...] = gate
        up_ref[...] = up
        hidden_ref[...] = hidden
        lora_gate_ref[...] = lora_gate
        lora_up_ref[...] = lora_up
        down_lora_ref[...] = dot(hidden, seconds[2 * rank :, :], 1, 1).astype(bf16)


def weight_specs(count, units, width, block, which=0):
    own = pl.BlockSpec((1, units, width), lambda g, s: (s[0], 0, s[1 + block(g)]))
    moved = pl.BlockSpec((units, width), lambda g, s: (which, s[1 + block(g)]))
    return [own] + [moved] * (count - 1)


def expert_forward(scalars, parts, gates, ups, firsts, seconds):
    rows, width = parts[0].shape
    rank, units = seconds.shape[0] // 3, seconds.shape[1]
    piece = units // 4
    block = lambda g: g
    specs = [whole((rows, width))] * 4
    specs += weight_specs(4, piece, width, block, 0) + weight_specs(4, piece, width, block, 1)
    specs += weight_specs(1, rank, width, block) * 2
    specs += [whole(seconds.shape)]
    shapes = [((rows, units), f32)] * 2 + [((rows, units), bf16)] + [((rows, rank), bf16)] * 3
    return pl.pallas_call(
        forward_kernel,
        grid_spec=pltpu.PrefetchScalarGridSpec(
            num_scalar_prefetch=1,
            grid=(4,),
            in_specs=specs,
            out_specs=[whole(shape) for shape, _ in shapes],
            scratch_shapes=[pltpu.VMEM((rows, 2 * units + 2 * rank), f32)],
        ),
        out_shape=[jax.ShapeDtypeStruct(shape, dtype) for shape, dtype in shapes],
        name="expert_forward",
    )(scalars, *parts, *gates, *ups, *firsts, seconds)


def backward_kernel(scalars, *refs):
    cots, parts, downs, refs = refs[:4], refs[4:8], refs[8:13], refs[13:]
    gates, ups, firsts, seconds, refs = refs[:4], refs[4:8], refs[8:10], refs[10], refs[11:]
    gate_ref, up_ref, hidden_ref, lora_gate_ref, lora_up_ref, down_lora_ref, *refs = refs
    own_ref, cross_ref, feature_ref, by_hidden_ref, acc, left = refs
    step = pl.program_id(0)
    rank = seconds.shape[0] // 3
    units = seconds.shape[1]

    @pl.when(step < 4)
    def _():
        weights = stack(downs)
        for k in range(4):

            @pl.when(step == k)
            def _(k=k):
                product = dot(cots[k][...], weights, 1, 1)
                acc[...] = product if k == 0 else acc[...] + product

    @pl.when(step == 3)
    def _():
        gate, up = gate_ref[...], up_ref[...]
        back_lora = acc[:, units:].astype(bf16)
        grad_hidden = acc[:, :units] + SCALE * dot(back_lora, seconds[2 * rank :, :], 1, 0)
        sigma = jax.nn.sigmoid(gate)
        grad_gate = (grad_hidden * up * sigma * (1.0 + gate * (1.0 - sigma))).astype(bf16)
        grad_up = (grad_hidden * (gate * sigma)).astype(bf16)
        left[:, :units] = grad_gate
        left[:, units : 2 * units] = grad_up
        gate_back = dot(grad_gate, seconds[:rank, :], 1, 1)
        up_back = dot(grad_up, seconds[rank : 2 * rank, :], 1, 1)
        left[:, 2 * units :] = (
            jnp.concatenate((gate_back, up_back), axis=1).astype(bf16).astype(f32) * SCALE
        ).astype(bf16)
        by_hidden_ref[:rank, :] = SCALE * dot(lora_gate_ref[...], grad_gate, 0, 0)
        by_hidden_ref[rank : 2 * rank, :] = SCALE * dot(lora_up_ref[...], grad_up, 0, 0)
        by_hidden_ref[2 * rank :, :] = SCALE * dot(back_lora, hidden_ref[...], 0, 0)

    @pl.when(step >= 4)
    def _():
        weights = stack((*gates, *ups, *firsts))
        result = dot(left[...], weights, 1, 0).astype(bf16)
        for k in range(4):

            @pl.when(step == 4 + k)
            def _(k=k):
                (own_ref, cross_ref)[k % 2][0] = result
                feature_ref[: 2 * rank, :] = dot(left[:, 2 * units :], parts[k][...], 0, 0)
                feature_ref[2 * rank :, :] = SCALE * dot(down_lora_ref[...], cots[k][...], 0, 0)


def expert_backward(scalars, cots, parts, downs, down_second, gates, ups, firsts, seconds, saved):
    rows, width = parts[0].shape
    rank, units = seconds.shape[0] // 3, seconds.shape[1]
    piece = units // 4
    early = lambda g: jnp.minimum(g, 3)
    late = lambda g: jnp.maximum(g - 4, 0)
    specs = [whole((rows, width))] * 8
    specs += weight_specs(4, piece, width, early, 2) + weight_specs(1, rank, width, early)
    specs += weight_specs(4, piece, width, late, 0) + weight_specs(4, piece, width, late, 1)
    specs += weight_specs(1, rank, width, late) * 2
    specs += [whole(seconds.shape)] + [whole(s.shape) for s in saved]
    return pl.pallas_call(
        backward_kernel,
        grid_spec=pltpu.PrefetchScalarGridSpec(
            num_scalar_prefetch=1,
            grid=(8,),
            in_specs=specs,
            out_specs=[
                pl.BlockSpec((1, rows, width), lambda g, s: (late(g) // 2, 0, 0)),
                pl.BlockSpec((1, rows, width), lambda g, s: (late(g) // 2, 0, 0)),
                pl.BlockSpec((3 * rank, width), lambda g, s: (0, late(g))),
                whole((3 * rank, units)),
            ],
            scratch_shapes=[
                pltpu.VMEM((rows, units + rank), f32),
                pltpu.VMEM((rows, 2 * units + 2 * rank), bf16),
            ],
        ),
        out_shape=[
            jax.ShapeDtypeStruct((2, rows, width), bf16),
            jax.ShapeDtypeStruct((2, rows, width), bf16),
            jax.ShapeDtypeStruct((3 * rank, 4 * width), f32),
            jax.ShapeDtypeStruct((3 * rank, units), f32),
        ],
        name="expert_backward",
    )(scalars, *cots, *parts, *downs, down_second, *gates, *ups, *firsts, seconds, *saved)


def local(
    tokens,
    grad_out,
    route_weights,
    expert_ids,
    gate_weight,
    up_weight,
    down_weight,
    gate_adapter_first,
    gate_adapter_second,
    up_adapter_first,
    up_adapter_second,
    down_adapter_first,
    down_adapter_second,
):
    e_index = lax.axis_index("expert")
    t_index = lax.axis_index("tensor")
    xl = e_index // (NZ * NY)
    z = (e_index // NY) % NZ
    y = e_index % NY
    xh = t_index // 2
    c = t_index % 2
    rows, width = tokens.shape
    features = [2 * (xh ^ i) + (c ^ j) for i in range(2) for j in range(2)]
    scalars = jnp.stack([xh, *features, xl ^ c, y, z, xl]).astype(jnp.int32)

    gate_t = jnp.swapaxes(gate_weight, 1, 2)
    up_t = jnp.swapaxes(up_weight, 1, 2)
    first_t = jnp.swapaxes(down_adapter_first, 1, 2)

    def of_expert(e, weights):
        big = jnp.concatenate([pick(w, e) for w in weights], axis=0)
        seconds = (gate_adapter_second, up_adapter_second, first_t)
        return big, jnp.concatenate([pick(w, e) for w in seconds], axis=0)

    big, small = of_expert(1 - xh, (gate_t, up_t, down_weight))
    big_x, small_x = move(big, X_HALF), move(small, X_HALF)

    ids_t = expert_ids.T.astype(bf16)
    w_t = route_weights.T
    w_hi = lax.reduce_precision(w_t, 8, 7)
    w_rest = w_t - w_hi
    w_mid = lax.reduce_precision(w_rest, 8, 7)
    w_low = w_rest - w_mid
    meta = jnp.concatenate(
        (ids_t, w_hi.astype(bf16), w_mid.astype(bf16), w_low.astype(bf16)), axis=1
    )
    packed = jnp.concatenate((tokens, meta), axis=0)

    z_shifts = (2, 6, 4, 1, 3, 7, 5)
    all_packed = [packed] + [move(packed, Z_BY[s]) for s in z_shifts]
    all_grad = [grad_out] + [move(grad_out, Z_BY[s]) for s in z_shifts]

    def to_chip(routed):
        return [routed[0]] + [move(routed[s], Y_BY[s]) for s in range(1, NY)]

    def over_x(got):
        sent = regroup(to_chips_kernel, got)
        return [sent[0]] + [move(sent[k], X_BY[k]) for k in range(1, 4)]

    def to_core(sent):
        n = sent[0].shape[0]
        crossed, kept_0, kept_1 = split(scalars, sent)
        crossed = move(crossed, CORE)
        return [kept_0, crossed[:n], kept_1, crossed[n:]]

    *chosen, in_0, in_1, in_2, in_3 = select_in(scalars, all_packed, rows, width)
    selects, row_weights = chosen[:2], chosen[2:]

    in_0, gate_own, up_own, down_own = lax.optimization_barrier((in_0, gate_t, up_t, down_weight))
    big_own, small_own = of_expert(xh, (gate_own, up_own, down_own))
    big_c, small_c = move(big_own, CORE), move(small_own, CORE)

    in_sent = over_x(to_chip((in_0, in_1, in_2, in_3)))
    grad_out_0, *grad_rest = select_grad(selects, row_weights, all_grad, width)
    grad_got = to_chip((grad_out_0, *grad_rest))
    big_xc, small_xc = move(big_x, CORE), move(small_x, CORE)
    gates, ups, downs = ((w, big_x, big_c, big_xc) for w in (gate_t, up_t, down_weight))
    seconds = jnp.concatenate((small_own, small_x, small_c, small_xc), axis=1)
    firsts = (jnp.swapaxes(gate_adapter_first, 1, 2), jnp.swapaxes(up_adapter_first, 1, 2))

    in_parts = to_core(in_sent)
    grad_sent = over_x(grad_got)

    saved = expert_forward(scalars, in_parts, gates, ups, firsts, seconds)
    tied = lax.optimization_barrier((*grad_sent, *saved))
    grad_sent, saved = tied[:4], tied[4:]
    grad_parts = to_core(grad_sent)
    own_grad, cross_grad, by_feature, by_hidden = expert_backward(
        scalars, grad_parts, in_parts, downs, down_adapter_second, gates, ups, firsts, seconds, saved
    )

    home = join(scalars, own_grad, move(cross_grad, CORE))
    home = [home[0]] + [move(home[k], X_BY[k]) for k in range(1, 4)]

    by_feature, by_hidden, *home = lax.optimization_barrier((by_feature, by_hidden, *home))

    units = gate_weight.shape[2]
    feature = [by_feature[:, k * width : (k + 1) * width] for k in range(4)]
    mine = jnp.concatenate((feature[0], feature[2], by_hidden[:, : 2 * units]), axis=1)
    other = jnp.concatenate((feature[1], feature[3], by_hidden[:, 2 * units :]), axis=1)
    total = mine + move(other, CORE)
    keep = jnp.concatenate(
        (total[:, :width], total[:, 2 * width : 2 * width + units]), axis=1
    )
    give = jnp.concatenate((total[:, width : 2 * width], total[:, 2 * width + units :]), axis=1)
    came = move(give, X_HALF)
    first = jnp.where(xh == 0, keep, came)
    second = jnp.where(xh == 0, came, keep)
    both = jnp.stack((first, second), axis=0)
    f_part, h_part = both[:, :, :width], both[:, :, width:]

    came_y = regroup(from_chips_kernel, home)
    came_y = [came_y[0]] + [move(came_y[s], inverse(Y_BY[s])) for s in range(1, NY)]
    down_pair, up_pair, far, near = combine(selects, came_y, rows, width)
    far = move(far, Z_BY[4])
    from_up = move(down_pair, Z_BY[7]).astype(f32)
    from_down = move(up_pair, Z_BY[1]).astype(f32)
    to_low = (near[rows : 2 * rows] + from_up[rows:]).astype(bf16)
    to_high = (near[2 * rows :] + from_down[rows:]).astype(bf16)
    result = near[:rows] + from_up[:rows] + from_down[:rows] + far.astype(f32)
    result = result + move(to_low, Z_BY[6]).astype(f32) + move(to_high, Z_BY[2]).astype(f32)
    return (
        result.astype(bf16),
        jnp.swapaxes(f_part[:, :64], 1, 2),
        h_part[:, :64],
        jnp.swapaxes(f_part[:, 64:128], 1, 2),
        h_part[:, 64:128],
        jnp.swapaxes(h_part[:, 128:], 1, 2),
        f_part[:, 128:],
    )


def solution(mesh):
    return jax.shard_map(
        local,
        mesh=mesh,
        in_specs=(
            P("expert", "tensor"),
            P("expert", "tensor"),
            P("expert", None),
            P("expert", None),
            P("expert", None, "tensor"),
            P("expert", None, "tensor"),
            P("expert", "tensor", None),
            P("expert", None, None),
            P("expert", None, "tensor"),
            P("expert", None, None),
            P("expert", None, "tensor"),
            P("expert", "tensor", None),
            P("expert", None, None),
        ),
        out_specs=(
            P("expert", "tensor"),
            P("expert", "tensor", None),
            P("expert", None, "tensor"),
            P("expert", "tensor", None),
            P("expert", None, "tensor"),
            P("expert", "tensor", None),
            P("expert", None, "tensor"),
        ),
        check_vma=False,
    )
```

```python
import jax
import jax.numpy as jnp
from jax import lax
from jax.experimental import pallas as pl
from jax.experimental.pallas import tpu as pltpu
from jax.sharding import PartitionSpec as P


bf16 = jnp.bfloat16
f32 = jnp.float32
SCALE = 0.5
NZ, NY, CAP, TOP = 8, 4, 12, 8
AXES = ("expert", "tensor")
HALF = CAP * NZ // 2


def pairs(fn):
    out = []
    for xl in range(2):
        for z in range(NZ):
            for y in range(NY):
                for xh in range(2):
                    for c in range(2):
                        a, b, d, e, f = fn(xl, z, y, xh, c)
                        src = ((xl * NZ + z) * NY + y) * 4 + xh * 2 + c
                        dst = ((a * NZ + b) * NY + d) * 4 + e * 2 + f
                        out.append((src, dst))
    return out


def inverse(perm):
    return [(d, s) for s, d in perm]


Z_BY = [pairs(lambda xl, z, y, xh, c, s=s: (xl, (z + s) % NZ, y, xh, c)) for s in range(NZ)]
Y_BY = [pairs(lambda xl, z, y, xh, c, s=s: (xl, z, (y + s) % NY, xh, c)) for s in range(NY)]
X_BY = [
    pairs(lambda xl, z, y, xh, c, i=i, j=j: (xl ^ j, z, y, xh ^ i, c))
    for i in range(2)
    for j in range(2)
]
X_HALF = pairs(lambda xl, z, y, xh, c: (xl, z, y, 1 - xh, c))
CORE = pairs(lambda xl, z, y, xh, c: (xl, z, y, xh, 1 - c))


def move(x, perm):
    return lax.ppermute(x, AXES, perm)


def dot(a, b, ca, cb):
    return lax.dot_general(a, b, (((ca,), (cb,)), ((), ())), preferred_element_type=f32)


def pick(array, index):
    return lax.dynamic_index_in_dim(array, index, 0, keepdims=False)


VMEM = pl.BlockSpec(memory_space=pltpu.VMEM)


def grant(mib):
    return pltpu.CompilerParams(vmem_limit_bytes=mib << 20)


def blocks_of(refs):
    n = refs[0].shape[0]
    starts = ((0, 0), (1, 0), (2, 0), (3, 0), (4, 0), (4, n), (5, 0), (5, n))
    return [(refs[k], start) for k, start in starts]


def select_kernel(scalars, *refs):
    packed, (*outs, target_ref, slot_weight_ref) = blocks_of(refs[:6]), refs[6:]
    select_refs, weight_refs, out_refs = outs[:2], outs[2:4], outs[4:]
    rows = (refs[0].shape[0] - TOP) // 2
    q = lax.broadcasted_iota(jnp.int32, (16, rows), 0)
    q_y = jnp.bitwise_and(scalars[6] + jnp.right_shift(q, 2), NY - 1)
    q_xh = jnp.bitwise_xor(scalars[0], jnp.bitwise_and(jnp.right_shift(q, 1), 1))
    q_xl = jnp.bitwise_xor(scalars[8], jnp.bitwise_and(q, 1))
    number = (2 * ((q_xl * NZ + scalars[7]) * NY + q_y) + q_xh).astype(f32)
    earlier = (
        lax.broadcasted_iota(jnp.int32, (rows, rows), 0)
        < lax.broadcasted_iota(jnp.int32, (rows, rows), 1)
    ).astype(f32).astype(bf16)
    for b in range(NZ):
        ref, start = packed[b]
        meta = ref[start + 2 * rows : start + 2 * rows + TOP, :].astype(f32)
        ids = meta[:, :rows]
        weight = meta[:, rows : 2 * rows] + meta[:, 2 * rows : 3 * rows] + meta[:, 3 * rows :]
        picked = jnp.zeros(number.shape, f32)
        slot_weight = jnp.zeros(number.shape, f32)
        for k in range(TOP):
            match = ids[k : k + 1, :] == number
            picked = jnp.where(match, 1.0, picked)
            slot_weight = jnp.where(match, weight[k : k + 1, :], slot_weight)
        before = dot(picked.astype(bf16), earlier, 1, 0)
        target = jnp.where(picked > 0.0, before + float(CAP * (b % 4)), -1.0)
        for q in range(16):
            target_ref[q, :, b * rows : (b + 1) * rows] = target[q : q + 1, :]
            slot_weight_ref[q, :, b * rows : (b + 1) * rows] = slot_weight[q : q + 1, :]
    place = lax.broadcasted_iota(jnp.int32, (HALF, rows), 0).astype(f32)

    def expert(q, _):
        start = pl.multiple_of(q * HALF, HALF)
        for h in range(2):
            total = jnp.zeros((HALF, rows), f32)
            for b in range(4):
                lanes = slice((4 * h + b) * rows, (4 * h + b + 1) * rows)
                hit = target_ref[q, :, lanes] == place
                select_refs[h][pl.ds(start, HALF), b * rows : (b + 1) * rows] = jnp.where(
                    hit, 1.0, 0.0
                ).astype(bf16)
                total = total + jnp.where(hit, slot_weight_ref[q, :, lanes], 0.0)
            weight_refs[h][pl.ds(start, HALF), :] = jnp.broadcast_to(
                jnp.sum(total, axis=1, keepdims=True), (HALF, rows)
            )
        return 0

    lax.fori_loop(0, 16, expert, 0)
    for h in range(2):
        every = jnp.concatenate(
            [p[start : start + rows, :] for p, start in packed[4 * h : 4 * h + 4]], axis=0
        )
        for s in range(NY):
            part = dot(select_refs[h][s * 4 * HALF : (s + 1) * 4 * HALF, :], every, 1, 0)
            out_refs[s][h * 4 * HALF : (h + 1) * 4 * HALF, :] = part.astype(bf16)


def select_in(scalars, packed, rows, width):
    slots = 16 * HALF
    shapes = [((slots, 4 * rows), bf16)] * 2 + [((slots, rows), f32)] * 2
    shapes += [((8 * HALF, width), bf16)] * NY
    return pl.pallas_call(
        select_kernel,
        in_specs=[SCALARS] + [VMEM] * 6,
        out_specs=[VMEM] * len(shapes),
        out_shape=[jax.ShapeDtypeStruct(shape, dtype) for shape, dtype in shapes],
        scratch_shapes=[pltpu.VMEM((16, 1, NZ * rows), f32), pltpu.VMEM((16, 1, NZ * rows), f32)],
        compiler_params=grant(16),
        name="select_in",
    )(scalars, *packed)


def select_grad_kernel(*refs):
    select_refs, weight_refs, out_refs = refs[:2], refs[2:4], refs[10:]
    packed = blocks_of(refs[4:10])
    rows = (refs[4].shape[0] - TOP) // 2
    for h in range(2):
        every = jnp.concatenate(
            [p[start + rows : start + 2 * rows, :] for p, start in packed[4 * h : 4 * h + 4]],
            axis=0,
        )
        for s in range(NY):
            part = slice(s * 4 * HALF, (s + 1) * 4 * HALF)
            product = dot(select_refs[h][part, :], every, 1, 0) * weight_refs[h][part, :1]
            out_refs[s][h * 4 * HALF : (h + 1) * 4 * HALF, :] = product.astype(bf16)


def select_grad(selects, weights, packed, width):
    return pl.pallas_call(
        select_grad_kernel,
        in_specs=[VMEM] * 10,
        out_specs=[VMEM] * NY,
        out_shape=[jax.ShapeDtypeStruct((8 * HALF, width), bf16) for _ in range(NY)],
        compiler_params=grant(16),
        name="select_grad",
    )(*selects, *weights, *packed)


def combine_kernel(*refs):
    select_refs, pieces, (down_ref, up_ref, far_ref, near_ref) = refs[:2], refs[2:6], refs[6:]
    half = near_ref.shape[0] // 3
    for h in (1, 0):
        values = jnp.concatenate(
            [p[h * 4 * HALF : (h + 1) * 4 * HALF, :] for p in pieces], axis=0
        )
        total = dot(select_refs[h][...], values, 0, 0)
        if h == 1:
            down_ref[...] = total[: 2 * half, :].astype(bf16)
            up_ref[...] = total[2 * half :, :].astype(bf16)
        else:
            near_ref[...] = total[: 3 * half, :]
            far_ref[...] = total[3 * half :, :].astype(bf16)


def combine(selects, pieces, rows, width):
    shapes = [((2 * rows, width), bf16)] * 2 + [((rows, width), bf16), ((3 * rows, width), f32)]
    return pl.pallas_call(
        combine_kernel,
        in_specs=[VMEM] * 6,
        out_specs=[VMEM] * 4,
        out_shape=[jax.ShapeDtypeStruct(shape, dtype) for shape, dtype in shapes],
        compiler_params=grant(16),
        name="combine",
    )(*selects, *pieces)


SCALARS = pl.BlockSpec(memory_space=pltpu.SMEM)


def to_chips_kernel(*refs):
    for s in range(NY):
        for h in range(2):
            for k in range(4):
                refs[4 + k][(2 * s + h) * HALF : (2 * s + h + 1) * HALF, :] = refs[s][
                    (4 * h + k) * HALF : (4 * h + k + 1) * HALF, :
                ]


def from_chips_kernel(*refs):
    for s in range(NY):
        for h in range(2):
            for k in range(4):
                refs[4 + s][(4 * h + k) * HALF : (4 * h + k + 1) * HALF, :] = refs[k][
                    (2 * s + h) * HALF : (2 * s + h + 1) * HALF, :
                ]


def regroup(kernel, pieces):
    return pl.pallas_call(
        kernel,
        in_specs=[VMEM] * 4,
        out_specs=[VMEM] * 4,
        out_shape=[jax.ShapeDtypeStruct(p.shape, p.dtype) for p in pieces],
        compiler_params=grant(8),
    )(*pieces)


def split_kernel(scalars, *refs):
    sent, (cross_ref, kept_ref) = refs[:4], refs[4:]
    for swapped in range(2):

        @pl.when(scalars[5] == swapped)
        def _(swapped=swapped):
            for i in range(2):
                kept_ref[i] = sent[2 * i + swapped][...]
                cross_ref[i] = sent[2 * i + 1 - swapped][...]


def split(scalars, sent):
    shape = jax.ShapeDtypeStruct((2, *sent[0].shape), bf16)
    return pl.pallas_call(
        split_kernel,
        in_specs=[SCALARS] + [VMEM] * 4,
        out_specs=[VMEM] * 2,
        out_shape=[shape] * 2,
        compiler_params=grant(8),
        name="split_cores",
    )(scalars, *sent)


def join_kernel(scalars, own_ref, crossed_ref, *home):
    for swapped in range(2):

        @pl.when(scalars[5] == swapped)
        def _(swapped=swapped):
            for i in range(2):
                home[2 * i + swapped][...] = own_ref[i]
                home[2 * i + 1 - swapped][...] = crossed_ref[i]


def join(scalars, own, crossed):
    return pl.pallas_call(
        join_kernel,
        in_specs=[SCALARS, VMEM, VMEM],
        out_specs=[VMEM] * 4,
        out_shape=[jax.ShapeDtypeStruct(own.shape[1:], bf16)] * 4,
        compiler_params=grant(8),
        name="join_cores",
    )(scalars, own, crossed)


def whole(shape):
    return pl.BlockSpec(shape, lambda g, s: (0,) * len(shape))


def stack(refs):
    return jnp.concatenate([r[0] if len(r.shape) == 3 else r[...] for r in refs], axis=0)


def part_of(parts, step):
    return jnp.where(step % 2 == 0, parts[0][0], parts[1][0])


def part_specs(rows, width, block):
    return [pl.BlockSpec((1, rows, width), lambda g, s: (block(g) // 2, 0, 0))] * 2


def forward_kernel(scalars, *refs):
    parts, (gates, ups, firsts), seconds = refs[:2], (refs[2:6], refs[6:10], refs[10:12]), refs[12]
    gate_ref, up_ref, hidden_ref, lora_gate_ref, lora_up_ref, down_lora_ref, acc = refs[13:]
    step = pl.program_id(0)
    rank = seconds.shape[0] // 3
    units = seconds.shape[1]
    product = dot(part_of(parts, step), stack((*gates, *ups, *firsts)), 1, 1)
    acc[...] = jnp.where(step == 0, 0.0, acc[...]) + product

    @pl.when(step == 3)
    def _():
        lora_gate = acc[:, 2 * units : 2 * units + rank].astype(bf16)
        lora_up = acc[:, 2 * units + rank :].astype(bf16)
        gate = acc[:, :units] + SCALE * dot(lora_gate, seconds[:rank, :], 1, 0)
        up = acc[:, units : 2 * units] + SCALE * dot(lora_up, seconds[rank : 2 * rank, :], 1, 0)
        hidden = (gate * jax.nn.sigmoid(gate) * up).astype(bf16)
        gate_ref[...] = gate
        up_ref[...] = up
        hidden_ref[...] = hidden
        lora_gate_ref[...] = lora_gate
        lora_up_ref[...] = lora_up
        down_lora_ref[...] = dot(hidden, seconds[2 * rank :, :], 1, 1).astype(bf16)


def weight_specs(count, units, width, block, which=0):
    own = pl.BlockSpec((1, units, width), lambda g, s: (s[0], 0, s[1 + block(g)]))
    moved = pl.BlockSpec((units, width), lambda g, s: (which, s[1 + block(g)]))
    return [own] + [moved] * (count - 1)


def expert_forward(scalars, parts, gates, ups, firsts, seconds):
    rows, width = parts[0].shape[1:]
    rank, units = seconds.shape[0] // 3, seconds.shape[1]
    piece = units // 4
    block = lambda g: g
    specs = part_specs(rows, width, block)
    specs += weight_specs(4, piece, width, block, 0) + weight_specs(4, piece, width, block, 1)
    specs += weight_specs(1, rank, width, block) * 2
    specs += [whole(seconds.shape)]
    shapes = [((rows, units), f32)] * 2 + [((rows, units), bf16)] + [((rows, rank), bf16)] * 3
    return pl.pallas_call(
        forward_kernel,
        grid_spec=pltpu.PrefetchScalarGridSpec(
            num_scalar_prefetch=1,
            grid=(4,),
            in_specs=specs,
            out_specs=[whole(shape) for shape, _ in shapes],
            scratch_shapes=[pltpu.VMEM((rows, 2 * units + 2 * rank), f32)],
        ),
        out_shape=[jax.ShapeDtypeStruct(shape, dtype) for shape, dtype in shapes],
        compiler_params=grant(28),
        name="expert_forward",
    )(scalars, *parts, *gates, *ups, *firsts, seconds)


def backward_kernel(scalars, *refs):
    cots, parts, late_cots, downs, refs = refs[:2], refs[2:4], refs[4:6], refs[6:11], refs[11:]
    gates, ups, firsts, seconds, refs = refs[:4], refs[4:8], refs[8:10], refs[10], refs[11:]
    gate_ref, up_ref, hidden_ref, lora_gate_ref, lora_up_ref, down_lora_ref, *refs = refs
    own_ref, cross_ref, feature_ref, by_hidden_ref, acc, left = refs
    step = pl.program_id(0)
    rank = seconds.shape[0] // 3
    units = seconds.shape[1]

    @pl.when(step < 4)
    def _():
        product = dot(part_of(cots, step), stack(downs), 1, 1)
        acc[...] = jnp.where(step == 0, 0.0, acc[...]) + product

    @pl.when(step == 3)
    def _():
        gate, up = gate_ref[...], up_ref[...]
        back_lora = acc[:, units:].astype(bf16)
        grad_hidden = acc[:, :units] + SCALE * dot(back_lora, seconds[2 * rank :, :], 1, 0)
        sigma = jax.nn.sigmoid(gate)
        grad_gate = (grad_hidden * up * sigma * (1.0 + gate * (1.0 - sigma))).astype(bf16)
        grad_up = (grad_hidden * (gate * sigma)).astype(bf16)
        left[:, :units] = grad_gate
        left[:, units : 2 * units] = grad_up
        gate_back = dot(grad_gate, seconds[:rank, :], 1, 1)
        up_back = dot(grad_up, seconds[rank : 2 * rank, :], 1, 1)
        left[:, 2 * units :] = (
            jnp.concatenate((gate_back, up_back), axis=1).astype(bf16).astype(f32) * SCALE
        ).astype(bf16)
        by_hidden_ref[:rank, :] = SCALE * dot(lora_gate_ref[...], grad_gate, 0, 0)
        by_hidden_ref[rank : 2 * rank, :] = SCALE * dot(lora_up_ref[...], grad_up, 0, 0)
        by_hidden_ref[2 * rank :, :] = SCALE * dot(back_lora, hidden_ref[...], 0, 0)

    @pl.when(step >= 4)
    def _():
        weights = stack((*gates, *ups, *firsts))
        result = dot(left[...], weights, 1, 0).astype(bf16)
        for k, ref in enumerate((own_ref, cross_ref)):

            @pl.when(step % 2 == k)
            def _(ref=ref):
                ref[0] = result

        feature_ref[: 2 * rank, :] = dot(left[:, 2 * units :], part_of(parts, step), 0, 0)
        feature_ref[2 * rank :, :] = SCALE * dot(down_lora_ref[...], part_of(late_cots, step), 0, 0)


def expert_backward(scalars, cots, parts, downs, down_second, gates, ups, firsts, seconds, saved):
    rows, width = parts[0].shape[1:]
    rank, units = seconds.shape[0] // 3, seconds.shape[1]
    piece = units // 4
    early = lambda g: jnp.minimum(g, 3)
    late = lambda g: jnp.maximum(g - 4, 0)
    specs = part_specs(rows, width, early) + part_specs(rows, width, late) * 2
    specs += weight_specs(4, piece, width, early, 2) + weight_specs(1, rank, width, early)
    specs += weight_specs(4, piece, width, late, 0) + weight_specs(4, piece, width, late, 1)
    specs += weight_specs(1, rank, width, late) * 2
    specs += [whole(seconds.shape)] + [whole(s.shape) for s in saved]
    return pl.pallas_call(
        backward_kernel,
        grid_spec=pltpu.PrefetchScalarGridSpec(
            num_scalar_prefetch=1,
            grid=(8,),
            in_specs=specs,
            out_specs=[
                pl.BlockSpec((1, rows, width), lambda g, s: (late(g) // 2, 0, 0)),
                pl.BlockSpec((1, rows, width), lambda g, s: (late(g) // 2, 0, 0)),
                pl.BlockSpec((3 * rank, width), lambda g, s: (0, late(g))),
                whole((3 * rank, units)),
            ],
            scratch_shapes=[
                pltpu.VMEM((rows, units + rank), f32),
                pltpu.VMEM((rows, 2 * units + 2 * rank), bf16),
            ],
        ),
        out_shape=[
            jax.ShapeDtypeStruct((2, rows, width), bf16),
            jax.ShapeDtypeStruct((2, rows, width), bf16),
            jax.ShapeDtypeStruct((3 * rank, 4 * width), f32),
            jax.ShapeDtypeStruct((3 * rank, units), f32),
        ],
        compiler_params=grant(36),
        name="expert_backward",
    )(scalars, *cots, *parts, *cots, *downs, down_second, *gates, *ups, *firsts, seconds, *saved)


def local(
    tokens,
    grad_out,
    route_weights,
    expert_ids,
    gate_weight,
    up_weight,
    down_weight,
    gate_adapter_first,
    gate_adapter_second,
    up_adapter_first,
    up_adapter_second,
    down_adapter_first,
    down_adapter_second,
):
    e_index = lax.axis_index("expert")
    t_index = lax.axis_index("tensor")
    xl = e_index // (NZ * NY)
    z = (e_index // NY) % NZ
    y = e_index % NY
    xh = t_index // 2
    c = t_index % 2
    rows, width = tokens.shape
    features = [2 * (xh ^ i) + (c ^ j) for i in range(2) for j in range(2)]
    scalars = jnp.stack([xh, *features, xl ^ c, y, z, xl]).astype(jnp.int32)

    gate_t = jnp.swapaxes(gate_weight, 1, 2)
    up_t = jnp.swapaxes(up_weight, 1, 2)
    first_t = jnp.swapaxes(down_adapter_first, 1, 2)

    def of_expert(e, weights):
        seconds = (gate_adapter_second, up_adapter_second, first_t)
        small = jnp.concatenate([pick(w, e) for w in seconds], axis=1)
        small = jnp.pad(small, ((0, 0), (0, weights[0].shape[2] - small.shape[1])))
        return jnp.concatenate([*(pick(w, e) for w in weights), small], axis=0)

    big_x = move(of_expert(1 - xh, (gate_t, up_t, down_weight)), X_HALF)

    ids_t = expert_ids.T.astype(bf16)
    w_t = route_weights.T
    w_hi = lax.reduce_precision(w_t, 8, 7)
    w_rest = w_t - w_hi
    w_mid = lax.reduce_precision(w_rest, 8, 7)
    w_low = w_rest - w_mid
    meta = jnp.concatenate(
        (ids_t, w_hi.astype(bf16), w_mid.astype(bf16), w_low.astype(bf16)), axis=1
    )
    packed = jnp.concatenate((tokens, grad_out, meta), axis=0)
    low, high = move(packed, Z_BY[2]), move(packed, Z_BY[6])
    far = move(packed, Z_BY[4])
    after = move(jnp.concatenate((packed, low), axis=0), Z_BY[1])
    ahead = move(jnp.concatenate((packed, high), axis=0), Z_BY[7])
    everything = (packed, low, high, far, after, ahead)

    def to_chip(routed):
        return [routed[0]] + [move(routed[s], Y_BY[s]) for s in range(1, NY)]

    def over_x(got):
        sent = regroup(to_chips_kernel, got)
        return [sent[0]] + [move(sent[k], X_BY[k]) for k in range(1, 4)]

    def to_core(sent):
        crossed, kept = split(scalars, sent)
        return kept, move(crossed, CORE)

    *chosen, in_0, in_1, in_2, in_3 = select_in(scalars, everything, rows, width)
    selects, row_weights = chosen[:2], chosen[2:]

    in_0, gate_own, up_own, down_own = lax.optimization_barrier((in_0, gate_t, up_t, down_weight))
    big_own = of_expert(xh, (gate_own, up_own, down_own))
    big_c = move(big_own, CORE)

    in_sent = over_x(to_chip((in_0, in_1, in_2, in_3)))
    grad_out_0, *grad_rest = select_grad(selects, row_weights, everything, width)
    grad_got = to_chip((grad_out_0, *grad_rest))
    big_xc = move(big_x, CORE)
    gates, ups, downs = ((w, big_x, big_c, big_xc) for w in (gate_t, up_t, down_weight))
    units = gate_weight.shape[2]
    seconds = [
        jnp.concatenate(
            [w[3 * units :, k * units : (k + 1) * units] for w in (big_own, big_x, big_c, big_xc)],
            axis=1,
        )
        for k in range(3)
    ]
    seconds = jnp.concatenate(seconds, axis=0)
    firsts = (jnp.swapaxes(gate_adapter_first, 1, 2), jnp.swapaxes(up_adapter_first, 1, 2))

    in_parts = to_core(in_sent)
    grad_sent = over_x(grad_got)

    saved = expert_forward(scalars, in_parts, gates, ups, firsts, seconds)
    tied = lax.optimization_barrier((*grad_sent, *saved))
    grad_sent, saved = tied[:4], tied[4:]
    grad_parts = to_core(grad_sent)
    own_grad, cross_grad, by_feature, by_hidden = expert_backward(
        scalars, grad_parts, in_parts, downs, down_adapter_second, gates, ups, firsts, seconds, saved
    )

    home = join(scalars, own_grad, move(cross_grad, CORE))
    home = [home[0]] + [move(home[k], X_BY[k]) for k in range(1, 4)]

    by_feature, by_hidden, *home = lax.optimization_barrier((by_feature, by_hidden, *home))

    feature = [by_feature[:, k * width : (k + 1) * width] for k in range(4)]
    mine = jnp.concatenate((feature[0], feature[2], by_hidden[:, : 2 * units]), axis=1)
    other = jnp.concatenate((feature[1], feature[3], by_hidden[:, 2 * units :]), axis=1)
    total = mine + move(other, CORE)
    keep = jnp.concatenate(
        (total[:, :width], total[:, 2 * width : 2 * width + units]), axis=1
    )
    give = jnp.concatenate((total[:, width : 2 * width], total[:, 2 * width + units :]), axis=1)
    came = move(give, X_HALF)
    first = jnp.where(xh == 0, keep, came)
    second = jnp.where(xh == 0, came, keep)
    both = jnp.stack((first, second), axis=0)
    f_part, h_part = both[:, :, :width], both[:, :, width:]

    came_y = regroup(from_chips_kernel, home)
    came_y = [came_y[0]] + [move(came_y[s], inverse(Y_BY[s])) for s in range(1, NY)]
    down_pair, up_pair, far, near = combine(selects, came_y, rows, width)
    far = move(far, Z_BY[4])
    from_up = move(down_pair, Z_BY[7]).astype(f32)
    from_down = move(up_pair, Z_BY[1]).astype(f32)
    to_low = (near[rows : 2 * rows] + from_up[rows:]).astype(bf16)
    to_high = (near[2 * rows :] + from_down[rows:]).astype(bf16)
    result = near[:rows] + from_up[:rows] + from_down[:rows] + far.astype(f32)
    result = result + move(to_low, Z_BY[6]).astype(f32) + move(to_high, Z_BY[2]).astype(f32)
    return (
        result.astype(bf16),
        jnp.swapaxes(f_part[:, :64], 1, 2),
        h_part[:, :64],
        jnp.swapaxes(f_part[:, 64:128], 1, 2),
        h_part[:, 64:128],
        jnp.swapaxes(h_part[:, 128:], 1, 2),
        f_part[:, 128:],
    )


def solution(mesh):
    return jax.shard_map(
        local,
        mesh=mesh,
        in_specs=(
            P("expert", "tensor"),
            P("expert", "tensor"),
            P("expert", None),
            P("expert", None),
            P("expert", None, "tensor"),
            P("expert", None, "tensor"),
            P("expert", "tensor", None),
            P("expert", None, None),
            P("expert", None, "tensor"),
            P("expert", None, None),
            P("expert", None, "tensor"),
            P("expert", "tensor", None),
            P("expert", None, None),
        ),
        out_specs=(
            P("expert", "tensor"),
            P("expert", "tensor", None),
            P("expert", None, "tensor"),
            P("expert", "tensor", None),
            P("expert", None, "tensor"),
            P("expert", "tensor", None),
            P("expert", None, "tensor"),
        ),
        check_vma=False,
    )
```

```python
import jax
import jax.numpy as jnp
from jax import lax
from jax.experimental import pallas as pl
from jax.experimental.pallas import tpu as pltpu
from jax.sharding import PartitionSpec as P


bf16 = jnp.bfloat16
f32 = jnp.float32
SCALE = 0.5
NZ, NY, CAP, TOP = 8, 4, 12, 8
AXES = ("expert", "tensor")
HALF = CAP * NZ // 2


def pairs(fn):
    out = []
    for xl in range(2):
        for z in range(NZ):
            for y in range(NY):
                for xh in range(2):
                    for c in range(2):
                        a, b, d, e, f = fn(xl, z, y, xh, c)
                        src = ((xl * NZ + z) * NY + y) * 4 + xh * 2 + c
                        dst = ((a * NZ + b) * NY + d) * 4 + e * 2 + f
                        out.append((src, dst))
    return out


def inverse(perm):
    return [(d, s) for s, d in perm]


Z_BY = [pairs(lambda xl, z, y, xh, c, s=s: (xl, (z + s) % NZ, y, xh, c)) for s in range(NZ)]
Y_BY = [pairs(lambda xl, z, y, xh, c, s=s: (xl, z, (y + s) % NY, xh, c)) for s in range(NY)]
X_BY = [
    pairs(lambda xl, z, y, xh, c, i=i, j=j: (xl ^ j, z, y, xh ^ i, c))
    for i in range(2)
    for j in range(2)
]
X_HALF = pairs(lambda xl, z, y, xh, c: (xl, z, y, 1 - xh, c))
CORE = pairs(lambda xl, z, y, xh, c: (xl, z, y, xh, 1 - c))


def move(x, perm):
    return lax.ppermute(x, AXES, perm)


def dot(a, b, ca, cb):
    return lax.dot_general(a, b, (((ca,), (cb,)), ((), ())), preferred_element_type=f32)


def pick(array, index):
    return lax.dynamic_index_in_dim(array, index, 0, keepdims=False)


VMEM = pl.BlockSpec(memory_space=pltpu.VMEM)


def grant(mib):
    return pltpu.CompilerParams(vmem_limit_bytes=mib << 20)


def blocks_of(refs):
    n = refs[0].shape[0]
    starts = ((0, 0), (1, 0), (2, 0), (3, 0), (4, 0), (4, n), (5, 0), (5, n))
    return [(refs[k], start) for k, start in starts]


def select_kernel(scalars, *refs):
    packed, (*outs, target_ref, slot_weight_ref) = blocks_of(refs[:6]), refs[6:]
    select_refs, weight_refs, out_refs = outs[:2], outs[2:4], outs[4:]
    rows = (refs[0].shape[0] - TOP) // 2
    q = lax.broadcasted_iota(jnp.int32, (16, rows), 0)
    q_y = jnp.bitwise_and(scalars[6] + jnp.right_shift(q, 2), NY - 1)
    q_xh = jnp.bitwise_xor(scalars[0], jnp.bitwise_and(jnp.right_shift(q, 1), 1))
    q_xl = jnp.bitwise_xor(scalars[8], jnp.bitwise_and(q, 1))
    number = (2 * ((q_xl * NZ + scalars[7]) * NY + q_y) + q_xh).astype(f32)
    earlier = (
        lax.broadcasted_iota(jnp.int32, (rows, rows), 0)
        < lax.broadcasted_iota(jnp.int32, (rows, rows), 1)
    ).astype(f32).astype(bf16)
    for b in range(NZ):
        ref, start = packed[b]
        meta = ref[start + 2 * rows : start + 2 * rows + TOP, :].astype(f32)
        ids = meta[:, :rows]
        weight = meta[:, rows : 2 * rows] + meta[:, 2 * rows : 3 * rows] + meta[:, 3 * rows :]
        picked = jnp.zeros(number.shape, f32)
        slot_weight = jnp.zeros(number.shape, f32)
        for k in range(TOP):
            match = ids[k : k + 1, :] == number
            picked = jnp.where(match, 1.0, picked)
            slot_weight = jnp.where(match, weight[k : k + 1, :], slot_weight)
        before = dot(picked.astype(bf16), earlier, 1, 0)
        target = jnp.where(picked > 0.0, before + float(CAP * (b % 4)), -1.0)
        for q in range(16):
            target_ref[q, :, b * rows : (b + 1) * rows] = target[q : q + 1, :]
            slot_weight_ref[q, :, b * rows : (b + 1) * rows] = slot_weight[q : q + 1, :]
    place = lax.broadcasted_iota(jnp.int32, (HALF, rows), 0).astype(f32)

    def expert(q, _):
        start = pl.multiple_of(q * HALF, HALF)
        for h in range(2):
            total = jnp.zeros((HALF, rows), f32)
            for b in range(4):
                lanes = slice((4 * h + b) * rows, (4 * h + b + 1) * rows)
                hit = target_ref[q, :, lanes] == place
                select_refs[h][pl.ds(start, HALF), b * rows : (b + 1) * rows] = jnp.where(
                    hit, 1.0, 0.0
                ).astype(bf16)
                total = total + jnp.where(hit, slot_weight_ref[q, :, lanes], 0.0)
            weight_refs[h][pl.ds(start, HALF), :] = jnp.broadcast_to(
                jnp.sum(total, axis=1, keepdims=True), (HALF, rows)
            )
        return 0

    lax.fori_loop(0, 16, expert, 0)
    for h in range(2):
        every = jnp.concatenate(
            [p[start : start + rows, :] for p, start in packed[4 * h : 4 * h + 4]], axis=0
        )
        for s in range(NY):
            part = dot(select_refs[h][s * 4 * HALF : (s + 1) * 4 * HALF, :], every, 1, 0)
            out_refs[s][h * 4 * HALF : (h + 1) * 4 * HALF, :] = part.astype(bf16)


def select_in(scalars, packed, rows, width):
    slots = 16 * HALF
    shapes = [((slots, 4 * rows), bf16)] * 2 + [((slots, rows), f32)] * 2
    shapes += [((8 * HALF, width), bf16)] * NY
    return pl.pallas_call(
        select_kernel,
        in_specs=[SCALARS] + [VMEM] * 6,
        out_specs=[VMEM] * len(shapes),
        out_shape=[jax.ShapeDtypeStruct(shape, dtype) for shape, dtype in shapes],
        scratch_shapes=[pltpu.VMEM((16, 1, NZ * rows), f32), pltpu.VMEM((16, 1, NZ * rows), f32)],
        compiler_params=grant(16),
        name="select_in",
    )(scalars, *packed)


def select_grad_kernel(*refs):
    select_refs, weight_refs, out_refs = refs[:2], refs[2:4], refs[10:]
    packed = blocks_of(refs[4:10])
    rows = (refs[4].shape[0] - TOP) // 2
    for h in range(2):
        every = jnp.concatenate(
            [p[start + rows : start + 2 * rows, :] for p, start in packed[4 * h : 4 * h + 4]],
            axis=0,
        )
        for s in range(NY):
            part = slice(s * 4 * HALF, (s + 1) * 4 * HALF)
            product = dot(select_refs[h][part, :], every, 1, 0) * weight_refs[h][part, :1]
            out_refs[s][h * 4 * HALF : (h + 1) * 4 * HALF, :] = product.astype(bf16)


def select_grad(selects, weights, packed, width):
    return pl.pallas_call(
        select_grad_kernel,
        in_specs=[VMEM] * 10,
        out_specs=[VMEM] * NY,
        out_shape=[jax.ShapeDtypeStruct((8 * HALF, width), bf16) for _ in range(NY)],
        compiler_params=grant(16),
        name="select_grad",
    )(*selects, *weights, *packed)


def combine_kernel(*refs):
    select_refs, pieces, (down_ref, up_ref, far_ref, near_ref) = refs[:2], refs[2:6], refs[6:]
    half = near_ref.shape[0] // 3
    for h in (1, 0):
        values = jnp.concatenate(
            [p[h * 4 * HALF : (h + 1) * 4 * HALF, :] for p in pieces], axis=0
        )
        total = dot(select_refs[h][...], values, 0, 0)
        if h == 1:
            down_ref[...] = total[: 2 * half, :].astype(bf16)
            up_ref[...] = total[2 * half :, :].astype(bf16)
        else:
            near_ref[...] = total[: 3 * half, :]
            far_ref[...] = total[3 * half :, :].astype(bf16)


def combine(selects, pieces, rows, width):
    shapes = [((2 * rows, width), bf16)] * 2 + [((rows, width), bf16), ((3 * rows, width), f32)]
    return pl.pallas_call(
        combine_kernel,
        in_specs=[VMEM] * 6,
        out_specs=[VMEM] * 4,
        out_shape=[jax.ShapeDtypeStruct(shape, dtype) for shape, dtype in shapes],
        compiler_params=grant(16),
        name="combine",
    )(*selects, *pieces)


SCALARS = pl.BlockSpec(memory_space=pltpu.SMEM)


def to_chips_kernel(*refs):
    for s in range(NY):
        for h in range(2):
            for k in range(4):
                refs[4 + k][(2 * s + h) * HALF : (2 * s + h + 1) * HALF, :] = refs[s][
                    (4 * h + k) * HALF : (4 * h + k + 1) * HALF, :
                ]


def from_chips_kernel(*refs):
    for s in range(NY):
        for h in range(2):
            for k in range(4):
                refs[4 + s][(4 * h + k) * HALF : (4 * h + k + 1) * HALF, :] = refs[k][
                    (2 * s + h) * HALF : (2 * s + h + 1) * HALF, :
                ]


def regroup(kernel, pieces):
    return pl.pallas_call(
        kernel,
        in_specs=[VMEM] * 4,
        out_specs=[VMEM] * 4,
        out_shape=[jax.ShapeDtypeStruct(p.shape, p.dtype) for p in pieces],
        compiler_params=grant(8),
    )(*pieces)


def split_kernel(scalars, *refs):
    sent, (cross_ref, kept_ref) = refs[:4], refs[4:]
    for swapped in range(2):

        @pl.when(scalars[5] == swapped)
        def _(swapped=swapped):
            for i in range(2):
                kept_ref[i] = sent[2 * i + swapped][...]
                cross_ref[i] = sent[2 * i + 1 - swapped][...]


def split(scalars, sent):
    shape = jax.ShapeDtypeStruct((2, *sent[0].shape), bf16)
    return pl.pallas_call(
        split_kernel,
        in_specs=[SCALARS] + [VMEM] * 4,
        out_specs=[VMEM] * 2,
        out_shape=[shape] * 2,
        compiler_params=grant(8),
        name="split_cores",
    )(scalars, *sent)


def join_kernel(scalars, own_ref, crossed_ref, *home):
    for swapped in range(2):

        @pl.when(scalars[5] == swapped)
        def _(swapped=swapped):
            home[swapped][...] = own_ref[...]
            home[1 - swapped][...] = crossed_ref[...]


def join(scalars, own, crossed):
    return pl.pallas_call(
        join_kernel,
        in_specs=[SCALARS, VMEM, VMEM],
        out_specs=[VMEM] * 2,
        out_shape=[jax.ShapeDtypeStruct(own.shape, bf16)] * 2,
        compiler_params=grant(8),
        name="join_cores",
    )(scalars, own, crossed)


def whole(shape):
    return pl.BlockSpec(shape, lambda g, s: (0,) * len(shape))


def stack(refs):
    return jnp.concatenate([r[0] if len(r.shape) == 3 else r[...] for r in refs], axis=0)


def part_of(parts, step):
    return jnp.where(step % 2 == 0, parts[0][0], parts[1][0])


def part_specs(rows, width, block):
    return [pl.BlockSpec((1, rows, width), lambda g, s: (block(g) // 2, 0, 0))] * 2


def forward_kernel(scalars, *refs):
    parts, (gates, ups, firsts), seconds = refs[:2], (refs[2:6], refs[6:10], refs[10:12]), refs[12]
    gate_ref, up_ref, hidden_ref, lora_gate_ref, lora_up_ref, down_lora_ref, acc = refs[13:]
    step = pl.program_id(0)
    rank = seconds.shape[0] // 3
    units = seconds.shape[1]
    product = dot(part_of(parts, step), stack((*gates, *ups, *firsts)), 1, 1)
    acc[...] = jnp.where(step == 0, 0.0, acc[...]) + product

    @pl.when(step == 3)
    def _():
        lora_gate = acc[:, 2 * units : 2 * units + rank].astype(bf16)
        lora_up = acc[:, 2 * units + rank :].astype(bf16)
        gate = acc[:, :units] + SCALE * dot(lora_gate, seconds[:rank, :], 1, 0)
        up = acc[:, units : 2 * units] + SCALE * dot(lora_up, seconds[rank : 2 * rank, :], 1, 0)
        hidden = (gate * jax.nn.sigmoid(gate) * up).astype(bf16)
        gate_ref[...] = gate
        up_ref[...] = up
        hidden_ref[...] = hidden
        lora_gate_ref[...] = lora_gate
        lora_up_ref[...] = lora_up
        down_lora_ref[...] = dot(hidden, seconds[2 * rank :, :], 1, 1).astype(bf16)


def weight_specs(count, units, width, block, which=0):
    own = pl.BlockSpec((1, units, width), lambda g, s: (s[0], 0, s[1 + block(g)]))
    moved = pl.BlockSpec((units, width), lambda g, s: (which, s[1 + block(g)]))
    return [own] + [moved] * (count - 1)


def expert_forward(scalars, parts, gates, ups, firsts, seconds):
    rows, width = parts[0].shape[1:]
    rank, units = seconds.shape[0] // 3, seconds.shape[1]
    piece = units // 4
    block = lambda g: g
    specs = part_specs(rows, width, block)
    specs += weight_specs(4, piece, width, block, 0) + weight_specs(4, piece, width, block, 1)
    specs += weight_specs(1, rank, width, block) * 2
    specs += [whole(seconds.shape)]
    shapes = [((rows, units), f32)] * 2 + [((rows, units), bf16)] + [((rows, rank), bf16)] * 3
    return pl.pallas_call(
        forward_kernel,
        grid_spec=pltpu.PrefetchScalarGridSpec(
            num_scalar_prefetch=1,
            grid=(4,),
            in_specs=specs,
            out_specs=[whole(shape) for shape, _ in shapes],
            scratch_shapes=[pltpu.VMEM((rows, 2 * units + 2 * rank), f32)],
        ),
        out_shape=[jax.ShapeDtypeStruct(shape, dtype) for shape, dtype in shapes],
        compiler_params=grant(28),
        name="expert_forward",
    )(scalars, *parts, *gates, *ups, *firsts, seconds)


def backward_kernel(scalars, *refs):
    cots, parts, late_cots, downs, refs = refs[:2], refs[2:4], refs[4:6], refs[6:11], refs[11:]
    gates, ups, firsts, seconds, refs = refs[:4], refs[4:8], refs[8:10], refs[10], refs[11:]
    gate_ref, up_ref, hidden_ref, lora_gate_ref, lora_up_ref, down_lora_ref, *refs = refs
    own_ref, cross_ref, feature_ref, by_hidden_ref, left, acc = refs
    step = pl.program_id(0)
    rank = seconds.shape[0] // 3
    units = seconds.shape[1]

    @pl.when(step < 4)
    def _():
        product = dot(part_of(cots, step), stack(downs), 1, 1)
        acc[...] = jnp.where(step == 0, 0.0, acc[...]) + product

    @pl.when(step == 3)
    def _():
        gate, up = gate_ref[...], up_ref[...]
        back_lora = acc[:, units:].astype(bf16)
        grad_hidden = acc[:, :units] + SCALE * dot(back_lora, seconds[2 * rank :, :], 1, 0)
        sigma = jax.nn.sigmoid(gate)
        grad_gate = (grad_hidden * up * sigma * (1.0 + gate * (1.0 - sigma))).astype(bf16)
        grad_up = (grad_hidden * (gate * sigma)).astype(bf16)
        left[:, :units] = grad_gate
        left[:, units : 2 * units] = grad_up
        gate_back = dot(grad_gate, seconds[:rank, :], 1, 1)
        up_back = dot(grad_up, seconds[rank : 2 * rank, :], 1, 1)
        left[:, 2 * units :] = (
            jnp.concatenate((gate_back, up_back), axis=1).astype(bf16).astype(f32) * SCALE
        ).astype(bf16)
        by_hidden_ref[:rank, :] = SCALE * dot(lora_gate_ref[...], grad_gate, 0, 0)
        by_hidden_ref[rank : 2 * rank, :] = SCALE * dot(lora_up_ref[...], grad_up, 0, 0)
        by_hidden_ref[2 * rank :, :] = SCALE * dot(back_lora, hidden_ref[...], 0, 0)

    @pl.when(step >= 4)
    def _():
        by_block(
            step, parts, late_cots, gates, ups, firsts, left, down_lora_ref,
            own_ref, cross_ref, feature_ref,
        )


def by_block(step, parts, cots, gates, ups, firsts, left, down_lora, own_ref, cross_ref, feature_ref):
    rank = down_lora.shape[1]
    result = dot(left[...], stack((*gates, *ups, *firsts)), 1, 0).astype(bf16)
    for k, ref in enumerate((own_ref, cross_ref)):

        @pl.when(step % 2 == k)
        def _(ref=ref):
            ref[...] = result

    feature_ref[: 2 * rank, :] = dot(left[:, left.shape[1] - 2 * rank :], part_of(parts, step), 0, 0)
    feature_ref[2 * rank :, :] = SCALE * dot(down_lora[...], part_of(cots, step), 0, 0)


def rest_kernel(scalars, *refs):
    parts, cots, gates, ups, firsts = refs[:2], refs[2:4], refs[4:8], refs[8:12], refs[12:14]
    left, down_lora, *outs = refs[14:]
    by_block(pl.program_id(0), parts, cots, gates, ups, firsts, left, down_lora, *outs)


def expert_rest(scalars, cots, parts, gates, ups, firsts, left, down_lora):
    rows, width = parts[0].shape[1:]
    rank, units = down_lora.shape[1], left.shape[1] // 2 - down_lora.shape[1]
    piece = units // 4
    block = lambda g: g
    specs = part_specs(rows, width, block) * 2
    specs += weight_specs(4, piece, width, block, 0) + weight_specs(4, piece, width, block, 1)
    specs += weight_specs(1, rank, width, block) * 2 + [whole(left.shape), whole(down_lora.shape)]
    return pl.pallas_call(
        rest_kernel,
        grid_spec=pltpu.PrefetchScalarGridSpec(
            num_scalar_prefetch=1,
            grid=(2,),
            in_specs=specs,
            out_specs=[
                whole((rows, width)),
                whole((rows, width)),
                pl.BlockSpec((3 * rank, width), lambda g, s: (0, g)),
            ],
        ),
        out_shape=[
            jax.ShapeDtypeStruct((rows, width), bf16),
            jax.ShapeDtypeStruct((rows, width), bf16),
            jax.ShapeDtypeStruct((3 * rank, 2 * width), f32),
        ],
        compiler_params=grant(28),
        name="expert_rest",
    )(scalars, *parts, *cots, *gates, *ups, *firsts, left, down_lora)


def expert_backward(scalars, cots, parts, downs, down_second, gates, ups, firsts, seconds, saved):
    rows, width = parts[0].shape[1:]
    rank, units = seconds.shape[0] // 3, seconds.shape[1]
    piece = units // 4
    early = lambda g: jnp.minimum(g, 3)
    late = lambda g: 2 + jnp.maximum(g - 4, 0)
    specs = part_specs(rows, width, early) + part_specs(rows, width, late) * 2
    specs += weight_specs(4, piece, width, early, 2) + weight_specs(1, rank, width, early)
    specs += weight_specs(4, piece, width, late, 0) + weight_specs(4, piece, width, late, 1)
    specs += weight_specs(1, rank, width, late) * 2
    specs += [whole(seconds.shape)] + [whole(s.shape) for s in saved]
    return pl.pallas_call(
        backward_kernel,
        grid_spec=pltpu.PrefetchScalarGridSpec(
            num_scalar_prefetch=1,
            grid=(6,),
            in_specs=specs,
            out_specs=[
                whole((rows, width)),
                whole((rows, width)),
                pl.BlockSpec((3 * rank, width), lambda g, s: (0, late(g) - 2)),
                whole((3 * rank, units)),
                whole((rows, 2 * units + 2 * rank)),
            ],
            scratch_shapes=[
                pltpu.VMEM((rows, units + rank), f32),
            ],
        ),
        out_shape=[
            jax.ShapeDtypeStruct((rows, width), bf16),
            jax.ShapeDtypeStruct((rows, width), bf16),
            jax.ShapeDtypeStruct((3 * rank, 2 * width), f32),
            jax.ShapeDtypeStruct((3 * rank, units), f32),
            jax.ShapeDtypeStruct((rows, 2 * units + 2 * rank), bf16),
        ],
        compiler_params=grant(36),
        name="expert_backward",
    )(scalars, *cots, *parts, *cots, *downs, down_second, *gates, *ups, *firsts, seconds, *saved)


def local(
    tokens,
    grad_out,
    route_weights,
    expert_ids,
    gate_weight,
    up_weight,
    down_weight,
    gate_adapter_first,
    gate_adapter_second,
    up_adapter_first,
    up_adapter_second,
    down_adapter_first,
    down_adapter_second,
):
    e_index = lax.axis_index("expert")
    t_index = lax.axis_index("tensor")
    xl = e_index // (NZ * NY)
    z = (e_index // NY) % NZ
    y = e_index % NY
    xh = t_index // 2
    c = t_index % 2
    rows, width = tokens.shape
    features = [2 * (xh ^ i) + (c ^ j) for i in range(2) for j in range(2)]
    scalars = jnp.stack([xh, *features, xl ^ c, y, z, xl]).astype(jnp.int32)

    gate_t = jnp.swapaxes(gate_weight, 1, 2)
    up_t = jnp.swapaxes(up_weight, 1, 2)
    first_t = jnp.swapaxes(down_adapter_first, 1, 2)

    def of_expert(e, weights):
        seconds = (gate_adapter_second, up_adapter_second, first_t)
        small = jnp.concatenate([pick(w, e) for w in seconds], axis=1)
        small = jnp.pad(small, ((0, 0), (0, weights[0].shape[2] - small.shape[1])))
        return jnp.concatenate([*(pick(w, e) for w in weights), small], axis=0)

    big_x = move(of_expert(1 - xh, (gate_t, up_t, down_weight)), X_HALF)

    ids_t = expert_ids.T.astype(bf16)
    w_t = route_weights.T
    w_hi = lax.reduce_precision(w_t, 8, 7)
    w_rest = w_t - w_hi
    w_mid = lax.reduce_precision(w_rest, 8, 7)
    w_low = w_rest - w_mid
    meta = jnp.concatenate(
        (ids_t, w_hi.astype(bf16), w_mid.astype(bf16), w_low.astype(bf16)), axis=1
    )
    packed = jnp.concatenate((tokens, grad_out, meta), axis=0)
    low, high = move(packed, Z_BY[2]), move(packed, Z_BY[6])
    far = move(packed, Z_BY[4])
    after = move(jnp.concatenate((packed, low), axis=0), Z_BY[1])
    ahead = move(jnp.concatenate((packed, high), axis=0), Z_BY[7])
    everything = (packed, low, high, far, after, ahead)

    def to_chip(routed):
        return [routed[0]] + [move(routed[s], Y_BY[s]) for s in range(1, NY)]

    def over_x(got):
        sent = regroup(to_chips_kernel, got)
        return [sent[0]] + [move(sent[k], X_BY[k]) for k in range(1, 4)]

    def to_core(sent):
        crossed, kept = split(scalars, sent)
        return kept, move(crossed, CORE)

    *chosen, in_0, in_1, in_2, in_3 = select_in(scalars, everything, rows, width)
    selects, row_weights = chosen[:2], chosen[2:]

    in_0, gate_own, up_own, down_own = lax.optimization_barrier((in_0, gate_t, up_t, down_weight))
    big_own = of_expert(xh, (gate_own, up_own, down_own))
    big_c = move(big_own, CORE)

    in_sent = over_x(to_chip((in_0, in_1, in_2, in_3)))
    grad_out_0, *grad_rest = select_grad(selects, row_weights, everything, width)
    grad_got = to_chip((grad_out_0, *grad_rest))
    big_xc = move(big_x, CORE)
    gates, ups, downs = ((w, big_x, big_c, big_xc) for w in (gate_t, up_t, down_weight))
    units = gate_weight.shape[2]
    seconds = [
        jnp.concatenate(
            [w[3 * units :, k * units : (k + 1) * units] for w in (big_own, big_x, big_c, big_xc)],
            axis=1,
        )
        for k in range(3)
    ]
    seconds = jnp.concatenate(seconds, axis=0)
    firsts = (jnp.swapaxes(gate_adapter_first, 1, 2), jnp.swapaxes(up_adapter_first, 1, 2))

    in_parts = to_core(in_sent)
    grad_sent = over_x(grad_got)

    saved = expert_forward(scalars, in_parts, gates, ups, firsts, seconds)
    tied = lax.optimization_barrier((*grad_sent, *saved))
    grad_sent, saved = tied[:4], tied[4:]
    grad_parts = to_core(grad_sent)
    own_1, cross_1, feature_1, by_hidden, left = expert_backward(
        scalars, grad_parts, in_parts, downs, down_adapter_second, gates, ups, firsts, seconds, saved
    )

    own_0, cross_0, feature_0 = expert_rest(
        scalars, grad_parts, in_parts, gates, ups, firsts, left, saved[-1]
    )
    home_2, home_3 = join(scalars, own_1, move(cross_1, CORE))
    home_2, home_3 = move(home_2, X_BY[2]), move(home_3, X_BY[3])
    home_0, home_1 = join(scalars, own_0, move(cross_0, CORE))
    home = [home_0, move(home_1, X_BY[1]), home_2, home_3]
    feature_0, feature_1, by_hidden, *home = lax.optimization_barrier(
        (feature_0, feature_1, by_hidden, *home)
    )

    feature = [f[:, k * width : (k + 1) * width] for f in (feature_0, feature_1) for k in range(2)]
    mine = jnp.concatenate((feature[0], feature[2], by_hidden[:, : 2 * units]), axis=1)
    other = jnp.concatenate((feature[1], feature[3], by_hidden[:, 2 * units :]), axis=1)
    total = mine + move(other, CORE)
    keep = jnp.concatenate(
        (total[:, :width], total[:, 2 * width : 2 * width + units]), axis=1
    )
    give = jnp.concatenate((total[:, width : 2 * width], total[:, 2 * width + units :]), axis=1)
    came = move(give, X_HALF)
    first = jnp.where(xh == 0, keep, came)
    second = jnp.where(xh == 0, came, keep)
    both = jnp.stack((first, second), axis=0)
    f_part, h_part = both[:, :, :width], both[:, :, width:]

    came_y = regroup(from_chips_kernel, home)
    came_y = [came_y[0]] + [move(came_y[s], inverse(Y_BY[s])) for s in range(1, NY)]
    down_pair, up_pair, far, near = combine(selects, came_y, rows, width)
    far = move(far, Z_BY[4])
    from_up = move(down_pair, Z_BY[7]).astype(f32)
    from_down = move(up_pair, Z_BY[1]).astype(f32)
    to_low = (near[rows : 2 * rows] + from_up[rows:]).astype(bf16)
    to_high = (near[2 * rows :] + from_down[rows:]).astype(bf16)
    result = near[:rows] + from_up[:rows] + from_down[:rows] + far.astype(f32)
    result = result + move(to_low, Z_BY[6]).astype(f32) + move(to_high, Z_BY[2]).astype(f32)
    return (
        result.astype(bf16),
        jnp.swapaxes(f_part[:, :64], 1, 2),
        h_part[:, :64],
        jnp.swapaxes(f_part[:, 64:128], 1, 2),
        h_part[:, 64:128],
        jnp.swapaxes(h_part[:, 128:], 1, 2),
        f_part[:, 128:],
    )


def solution(mesh):
    return jax.shard_map(
        local,
        mesh=mesh,
        in_specs=(
            P("expert", "tensor"),
            P("expert", "tensor"),
            P("expert", None),
            P("expert", None),
            P("expert", None, "tensor"),
            P("expert", None, "tensor"),
            P("expert", "tensor", None),
            P("expert", None, None),
            P("expert", None, "tensor"),
            P("expert", None, None),
            P("expert", None, "tensor"),
            P("expert", "tensor", None),
            P("expert", None, None),
        ),
        out_specs=(
            P("expert", "tensor"),
            P("expert", "tensor", None),
            P("expert", None, "tensor"),
            P("expert", "tensor", None),
            P("expert", None, "tensor"),
            P("expert", "tensor", None),
            P("expert", None, "tensor"),
        ),
        check_vma=False,
    )
```
